16 devices in a mesh: fsdp: 16 (over z, y, x, core).
Axes of the slice: x: 2, y: 2, z: 2, core: 2. Of those that a mesh axis runs over, the one named last changes fastest.
Arguments:
- tokens: int32 [32, 512], P('fsdp')
- positions: int32 [32, 512], P('fsdp')
- embed_table: bfloat16 [152064, 1024], P('fsdp')
- attn_norm: bfloat16 [1024], P('fsdp')
- w_query: bfloat16 [1024, 2048], P('fsdp')
- w_key: bfloat16 [1024, 1024], P('fsdp')
- w_value: bfloat16 [1024, 1024], P('fsdp')
- q_norm: bfloat16 [128], replicated
- k_norm: bfloat16 [128], replicated
- w_out: bfloat16 [2048, 1024], P('fsdp')
- mlp_norm: bfloat16 [1024], P('fsdp')
- w_gate: bfloat16 [1024, 3072], P('fsdp')
- w_up: bfloat16 [1024, 3072], P('fsdp')
- w_down: bfloat16 [3072, 1024], P('fsdp')
- dy_out: bfloat16 [32, 512, 1024], P('fsdp')
Outputs:
- output 1: bfloat16 [32, 512, 1024], P('fsdp')
- output 2: float32 [152064, 1024], P('fsdp')
- output 3: float32 [1024], P('fsdp')
- output 4: float32 [1024, 2048], P('fsdp')
- output 5: float32 [1024, 1024], P('fsdp')
- output 6: float32 [1024, 1024], P('fsdp')
- output 7: float32 [128], replicated
- output 8: float32 [128], replicated
- output 9: float32 [2048, 1024], P('fsdp')
- output 10: float32 [1024], P('fsdp')
- output 11: float32 [1024, 3072], P('fsdp')
- output 12: float32 [1024, 3072], P('fsdp')
- output 13: float32 [3072, 1024], P('fsdp')
All inputs are finite; a program needn't handle non-finite values.
Results may differ from the reference program's by a relative error of at most 0.0158748.
Values are sent between devices in bfloat16 or wider.
A program may use at most 1 GiB of HBM per device.

```python
import math
import jax
import jax.numpy as jnp
from jax import lax

D = 1024
HEADS = 16
KV_HEADS = 8
HEAD = 128
FF = 3072
VOCAB = 151936
VOCAB_P = 152064
GROUP = 16
BATCH_DEV = 2
SEQ = 512

BATCH = GROUP * BATCH_DEV
Q_PER_KV = HEADS // KV_HEADS
ROWS_SHARD = VOCAB_P // GROUP
DOC_SPAN = max(SEQ // 4, 2)
NORM_EPS = 1e-6
ROPE_THETA = 1.0e6


def draw_tokens(rng_key):
    key_list = jax.random.split(rng_key, 4)
    id_top = jax.random.randint(key_list[0], (BATCH, SEQ), 1, VOCAB + 1)
    id_mid = jax.random.randint(key_list[1], (BATCH, SEQ), 0, id_top)
    token_ids = jax.random.randint(key_list[2], (BATCH, SEQ), 0, id_mid + 1)
    shard_lo = (jnp.arange(BATCH) % GROUP) * ROWS_SHARD
    shard_hi = jnp.minimum(shard_lo + ROWS_SHARD, VOCAB)
    cover_ids = jax.random.randint(key_list[3], (BATCH,), shard_lo, shard_hi)
    token_ids = token_ids.at[:, 0].set(cover_ids)
    return token_ids.at[BATCH - 1, SEQ - 1].set(VOCAB - 1).astype(jnp.int32)


def draw_positions(rng_key):
    seq_idx = jnp.arange(SEQ, dtype=jnp.int32)[None, :]
    starts = (jax.random.randint(rng_key, (BATCH, SEQ), 0, DOC_SPAN) == 0) | (seq_idx == 0)
    last_start = lax.cummax(jnp.where(starts, seq_idx, 0), axis=1)
    return (seq_idx - last_start).astype(jnp.int32)


def setup_inputs(seed: int = 0) -> dict:
    key_list = jax.random.split(jax.random.key(seed), 16)

    def weight(key_idx, arr_shape, fan_in):
        return (jax.random.normal(key_list[key_idx], arr_shape, jnp.float32) * fan_in ** -0.5).astype(jnp.bfloat16)

    def gain_vec(key_idx, vec_len):
        return (1.0 + 0.25 * jax.random.normal(key_list[key_idx], (vec_len,), jnp.float32)).astype(jnp.bfloat16)

    table_f = jax.random.normal(key_list[2], (VOCAB_P, D), jnp.float32)
    table_f = jnp.where(jnp.arange(VOCAB_P)[:, None] < VOCAB, table_f, 0.0)
    return {
        'tokens': draw_tokens(key_list[0]),
        'positions': draw_positions(key_list[1]),
        'embed_table': table_f.astype(jnp.bfloat16),
        'attn_norm': gain_vec(3, D),
        'w_query': weight(4, (D, HEADS * HEAD), D),
        'w_key': weight(5, (D, KV_HEADS * HEAD), D),
        'w_value': weight(6, (D, KV_HEADS * HEAD), D),
        'q_norm': gain_vec(7, HEAD),
        'k_norm': gain_vec(8, HEAD),
        'w_out': weight(9, (HEADS * HEAD, D), HEADS * HEAD),
        'mlp_norm': gain_vec(10, D),
        'w_gate': weight(11, (D, FF), D),
        'w_up': weight(12, (D, FF), D),
        'w_down': weight(13, (FF, D), FF),
        'dy_out': jax.random.normal(key_list[14], (BATCH, SEQ, D), jnp.float32).astype(jnp.bfloat16),
    }


def to_bf16(values):
    return values + lax.stop_gradient(values.astype(jnp.bfloat16).astype(jnp.float32) - values)


def rms_scale(values, norm_gain):
    inv_rms = lax.rsqrt(jnp.mean(values * values, axis=-1, keepdims=True) + NORM_EPS)
    return values * inv_rms * norm_gain


def rope_tables(positions):
    half_dim = HEAD // 2
    inv_freq = jnp.exp(jnp.arange(half_dim, dtype=jnp.float32) * (-2.0 * math.log(ROPE_THETA) / HEAD))
    angles = positions.astype(jnp.float32)[:, :, None] * inv_freq
    return jnp.cos(angles), jnp.sin(angles)


def rotate(values, cos_t, sin_t):
    half_dim = values.shape[-1] // 2
    lead_half = values[..., :half_dim]
    tail_half = values[..., half_dim:]
    return jnp.concatenate([lead_half * cos_t - tail_half * sin_t, tail_half * cos_t + lead_half * sin_t], axis=-1)


def seq_attend(operands):
    q_seq, k_seq, v_seq = operands
    scores = jnp.einsum('qgrh,kgh->grqk', q_seq, k_seq) * (HEAD ** -0.5)
    causal = jnp.arange(SEQ)[:, None] >= jnp.arange(SEQ)[None, :]
    scores = jnp.where(causal, scores, -1e30)
    attn_probs = to_bf16(jax.nn.softmax(scores, axis=-1))
    return to_bf16(jnp.einsum('grqk,kgh->qgrh', attn_probs, v_seq))


def reference(tokens, positions, embed_table, attn_norm, w_query, w_key, w_value, q_norm, k_norm, w_out, mlp_norm, w_gate, w_up, w_down, dy_out):
    cos_t, sin_t = rope_tables(positions)
    cos_q = cos_t[:, :, None, None, :]
    sin_q = sin_t[:, :, None, None, :]
    cos_k = cos_t[:, :, None, :]
    sin_k = sin_t[:, :, None, :]

    def layer_fwd(x_emb, g_attn, wt_query, wt_key, wt_value, g_query, g_key, wt_out, g_mlp, wt_gate, wt_up, wt_down):
        normed = to_bf16(rms_scale(x_emb, g_attn)).reshape(BATCH * SEQ, D)
        q_proj = to_bf16(jnp.dot(normed, wt_query, preferred_element_type=jnp.float32)).reshape(BATCH, SEQ, KV_HEADS, Q_PER_KV, HEAD)
        k_proj = to_bf16(jnp.dot(normed, wt_key, preferred_element_type=jnp.float32)).reshape(BATCH, SEQ, KV_HEADS, HEAD)
        v_proj = to_bf16(jnp.dot(normed, wt_value, preferred_element_type=jnp.float32)).reshape(BATCH, SEQ, KV_HEADS, HEAD)
        q_rot = to_bf16(rotate(rms_scale(q_proj, g_query), cos_q, sin_q))
        k_rot = to_bf16(rotate(rms_scale(k_proj, g_key), cos_k, sin_k))
        attn_heads = lax.map(jax.checkpoint(seq_attend), (q_rot, k_rot, v_proj))
        attn_proj = jnp.dot(attn_heads.reshape(BATCH * SEQ, HEADS * HEAD), wt_out, preferred_element_type=jnp.float32)
        hidden = to_bf16(x_emb + attn_proj.reshape(BATCH, SEQ, D))
        mlp_in = to_bf16(rms_scale(hidden, g_mlp)).reshape(BATCH * SEQ, D)
        gate_pre = jnp.dot(mlp_in, wt_gate, preferred_element_type=jnp.float32)
        up_proj = jnp.dot(mlp_in, wt_up, preferred_element_type=jnp.float32)
        mlp_act = to_bf16(jax.nn.silu(gate_pre) * up_proj)
        mlp_proj = jnp.dot(mlp_act, wt_down, preferred_element_type=jnp.float32)
        return to_bf16(hidden + mlp_proj.reshape(BATCH, SEQ, D))

    x_emb = jnp.take(embed_table, tokens, axis=0).astype(jnp.float32)
    params = [weight_arr.astype(jnp.float32) for weight_arr in (attn_norm, w_query, w_key, w_value, q_norm, k_norm, w_out, mlp_norm, w_gate, w_up, w_down)]
    layer_out, pullback = jax.vjp(layer_fwd, x_emb, *params)
    grad_list = pullback(dy_out.astype(jnp.float32))
    d_table = jax.ops.segment_sum(grad_list[0].reshape(BATCH * SEQ, D), tokens.reshape(BATCH * SEQ), num_segments=VOCAB_P)
    return (layer_out.astype(jnp.bfloat16), d_table, grad_list[1], grad_list[2], grad_list[3], grad_list[4], grad_list[5], grad_list[6], grad_list[7], grad_list[8], grad_list[9], grad_list[10], grad_list[11])
```

```python
import functools
import math
import jax
import jax.numpy as jnp
from jax import lax
from jax.experimental import pallas as pl
from jax.experimental.layout import Layout, with_layout_constraint
from jax.experimental.pallas import tpu as pltpu
from jax.sharding import PartitionSpec as P

NORM_EPS = 1e-6
ROPE_THETA = 1.0e6
AXIS_NAME = 'fsdp'
NEG = -1e30


def split_rows(a):
    return a.reshape(2, a.shape[0] // 2, a.shape[1])


def kdot_nn(a, b):
    return lax.dot_general(a, b, (((1,), (0,)), ((), ())), preferred_element_type=jnp.float32)


def kdot_nt(a, b):
    return lax.dot_general(a, b, (((1,), (1,)), ((), ())), preferred_element_type=jnp.float32)


def dot_nn(a, b):
    return lax.dot_general(split_rows(a), b, (((2,), (0,)), ((), ())), preferred_element_type=jnp.float32).reshape(a.shape[0], -1)


def dot_nt(a, b):
    return lax.dot_general(split_rows(a), b, (((2,), (1,)), ((), ())), preferred_element_type=jnp.float32).reshape(a.shape[0], -1)


def dot_tn(a, b):
    return lax.dot_general(split_rows(a), split_rows(b), (((0, 1), (0, 1)), ((), ())), preferred_element_type=jnp.float32)


def row_major(a):
    return with_layout_constraint(a, Layout(major_to_minor=tuple(range(a.ndim))))


def norm_fwd(values):
    values_f = values.astype(jnp.float32)
    inv_rms = lax.rsqrt(jnp.mean(values_f * values_f, axis=-1, keepdims=True) + NORM_EPS)
    return values_f * inv_rms, inv_rms


def norm_bwd(grad_out, normed, inv_rms, gain_f):
    grad_normed = grad_out * gain_f
    mean_term = jnp.mean(grad_normed * normed, axis=-1, keepdims=True)
    return inv_rms * (grad_normed - normed * mean_term)


def rope_tables(positions, head_dim):
    half_dim = head_dim // 2
    inv_freq = jnp.exp(jnp.arange(half_dim, dtype=jnp.float32) * (-2.0 * math.log(ROPE_THETA) / head_dim))
    angles = positions.astype(jnp.float32).reshape(-1, 1) * inv_freq
    cos_t, sin_t = jnp.cos(angles), jnp.sin(angles)
    return jnp.concatenate([cos_t, cos_t], axis=-1), jnp.concatenate([-sin_t, sin_t], axis=-1)


def rope(values, cos_t, sin_t):
    return values * cos_t + pltpu.roll(values, values.shape[-1] // 2, 1) * sin_t


def attn_fwd_kernel(n_rep, hd, chunk, qkv_ref, cos_ref, sin_ref, qg_ref, kg_ref, out_ref, *rep_refs):
    seq = qkv_ref.shape[0]
    scale = hd ** -0.5
    cos_t, sin_t = cos_ref[...], sin_ref[...]
    k_n, _ = norm_fwd(qkv_ref[:, n_rep * hd:(n_rep + 1) * hd])
    k_rot = rope(k_n * kg_ref[...], cos_t, sin_t).astype(jnp.bfloat16)
    v_raw = qkv_ref[:, (n_rep + 1) * hd:(n_rep + 2) * hd]
    for rep in range(n_rep):
        q_n, _ = norm_fwd(qkv_ref[:, rep * hd:(rep + 1) * hd])
        q_rot = rope(q_n * qg_ref[...], cos_t, sin_t).astype(jnp.bfloat16)
        for lo in range(0, seq, chunk):
            end = lo + chunk
            s = kdot_nt(q_rot[lo:end], k_rot[:end]) * scale
            rows = lax.broadcasted_iota(jnp.int32, s.shape, 0) + lo
            cols = lax.broadcasted_iota(jnp.int32, s.shape, 1)
            s = jnp.where(rows >= cols, s, NEG)
            e = jnp.exp(s - jnp.max(s, axis=-1, keepdims=True))
            p = e * (1.0 / jnp.sum(e, axis=-1, keepdims=True))
            o = kdot_nn(p.astype(jnp.bfloat16), v_raw[:end])
            out_ref[lo:end, rep * hd:(rep + 1) * hd] = o.astype(jnp.bfloat16)
            rep_refs[rep][lo:end] = o.astype(jnp.bfloat16)


def attn_fwd(qkv, cos_t, sin_t, q_gain, k_gain, batch, kv_heads, n_rep, hd):
    tokens, width = qkv.shape
    seq = tokens // batch
    gw = width // kv_heads
    return pl.pallas_call(
        functools.partial(attn_fwd_kernel, n_rep, hd, seq // 2),
        grid=(batch, kv_heads),
        in_specs=[pl.BlockSpec((seq, gw), lambda b, g: (b, g)),
                  pl.BlockSpec((seq, hd), lambda b, g: (b, 0)),
                  pl.BlockSpec((seq, hd), lambda b, g: (b, 0)),
                  pl.BlockSpec((1, hd), lambda b, g: (0, 0)),
                  pl.BlockSpec((1, hd), lambda b, g: (0, 0))],
        out_specs=[pl.BlockSpec((seq, n_rep * hd), lambda b, g: (b, g))] + [pl.BlockSpec((seq, hd), lambda b, g: (b, g))] * n_rep,
        out_shape=[jax.ShapeDtypeStruct((tokens, kv_heads * n_rep * hd), jnp.bfloat16)] + [jax.ShapeDtypeStruct((tokens, kv_heads * hd), jnp.bfloat16)] * n_rep,
        cost_estimate=pl.CostEstimate(flops=25_000_000_000, bytes_accessed=14_000_000, transcendentals=8_400_000),
        name='attn_fwd',
    )(qkv, cos_t, sin_t, q_gain, k_gain)


def attn_bwd_kernel(n_rep, hd, chunk, n_alias, qkv_ref, do_ref, cos_ref, sin_ref, qg_ref, kg_ref, *rest):
    dqkv_ref, dqg_ref, dkg_ref, dk_acc, dv_acc = rest[n_alias:]
    seq = qkv_ref.shape[0]
    scale = hd ** -0.5
    cos_t, sin_t = cos_ref[...], sin_ref[...]
    qg, kg = qg_ref[...], kg_ref[...]

    @pl.when(pl.program_id(0) == 0)
    def _():
        dqg_ref[...] = jnp.zeros_like(dqg_ref)
        dkg_ref[...] = jnp.zeros_like(dkg_ref)

    k_n, k_inv = norm_fwd(qkv_ref[:, n_rep * hd:(n_rep + 1) * hd])
    k_rot_f = rope(k_n * kg, cos_t, sin_t)
    k_rot = k_rot_f.astype(jnp.bfloat16)
    k_rot_t = k_rot_f.T.astype(jnp.bfloat16)
    v_raw = qkv_ref[:, (n_rep + 1) * hd:(n_rep + 2) * hd]
    dk_acc[...] = jnp.zeros_like(dk_acc)
    dv_acc[...] = jnp.zeros_like(dv_acc)
    for rep in range(n_rep):
        q_n, q_inv = norm_fwd(qkv_ref[:, rep * hd:(rep + 1) * hd])
        q_rot = rope(q_n * qg, cos_t, sin_t).astype(jnp.bfloat16)
        dq_parts = []
        for lo in range(0, seq, chunk):
            end = lo + chunk
            q_c = q_rot[lo:end]
            do_c = do_ref[lo:end, rep * hd:(rep + 1) * hd]
            s = kdot_nt(k_rot[:end], q_c) * scale
            keys = lax.broadcasted_iota(jnp.int32, s.shape, 0)
            qpos = lax.broadcasted_iota(jnp.int32, s.shape, 1) + lo
            s = jnp.where(qpos >= keys, s, NEG)
            e = jnp.exp(s - jnp.max(s, axis=0, keepdims=True))
            p = e * (1.0 / jnp.sum(e, axis=0, keepdims=True))
            dv_acc[:end] += kdot_nn(p.astype(jnp.bfloat16), do_c)
            dp = kdot_nt(v_raw[:end], do_c)
            delta = jnp.sum(dp * p, axis=0, keepdims=True)
            ds = (p * (dp - delta) * scale).astype(jnp.bfloat16)
            dk_acc[:end] += kdot_nn(ds, q_c)
            dq_parts.append(kdot_nn(k_rot_t[:, :end], ds).T)
        dq = jnp.concatenate(dq_parts, axis=0)
        dqt = dq * cos_t - pltpu.roll(dq, hd // 2, 1) * sin_t
        dqg_ref[...] += jnp.sum((dqt * q_n).reshape(seq // 8, 8, hd), axis=0)
        dqkv_ref[:, rep * hd:(rep + 1) * hd] = norm_bwd(dqt, q_n, q_inv, qg).astype(jnp.bfloat16)
    dk = dk_acc[...]
    dkt = dk * cos_t - pltpu.roll(dk, hd // 2, 1) * sin_t
    dkg_ref[...] += jnp.sum((dkt * k_n).reshape(seq // 8, 8, hd), axis=0)
    dqkv_ref[:, n_rep * hd:(n_rep + 1) * hd] = norm_bwd(dkt, k_n, k_inv, kg).astype(jnp.bfloat16)
    dqkv_ref[:, (n_rep + 1) * hd:(n_rep + 2) * hd] = dv_acc[...].astype(jnp.bfloat16)


def attn_bwd(b, prev, qkv, do, cos_t, sin_t, q_gain, k_gain, batch, kv_heads, n_rep, hd):
    tokens, width = qkv.shape
    seq = tokens // batch
    gw = width // kv_heads
    return pl.pallas_call(
        functools.partial(attn_bwd_kernel, n_rep, hd, seq // 2, len(prev)),
        grid=(kv_heads,),
        in_specs=[pl.BlockSpec((seq, gw), lambda g: (b, g)),
                  pl.BlockSpec((seq, n_rep * hd), lambda g: (b, g)),
                  pl.BlockSpec((seq, hd), lambda g: (b, 0)),
                  pl.BlockSpec((seq, hd), lambda g: (b, 0)),
                  pl.BlockSpec((1, hd), lambda g: (0, 0)),
                  pl.BlockSpec((1, hd), lambda g: (0, 0))] + [pl.BlockSpec(memory_space=pl.ANY)] * len(prev),
        out_specs=[pl.BlockSpec((seq, gw), lambda g: (b, g)),
                   pl.BlockSpec((8, hd), lambda g: (0, 0)),
                   pl.BlockSpec((8, hd), lambda g: (0, 0))],
        out_shape=[jax.ShapeDtypeStruct((tokens, width), jnp.bfloat16),
                   jax.ShapeDtypeStruct((8, hd), jnp.float32),
                   jax.ShapeDtypeStruct((8, hd), jnp.float32)],
        input_output_aliases={6: 0} if prev else {},
        scratch_shapes=[pltpu.VMEM((seq, hd), jnp.float32), pltpu.VMEM((seq, hd), jnp.float32)],
        cost_estimate=pl.CostEstimate(flops=25_000_000_000, bytes_accessed=14_000_000, transcendentals=4_200_000),
        name='attn_bwd',
    )(qkv, do, cos_t, sin_t, q_gain, k_gain, *prev)


def mlp_bwd_kernel(ff, gu_ref, ga_ref, out_ref, act_ref, act_t_ref):
    gate, up, grad_act = gu_ref[:, :ff], gu_ref[:, ff:], ga_ref[...]
    sig = jax.nn.sigmoid(gate)
    out_ref[:, :ff] = (grad_act * up * sig * (1.0 + gate * (1.0 - sig))).astype(jnp.bfloat16)
    out_ref[:, ff:] = (grad_act * gate * sig).astype(jnp.bfloat16)
    act = gate * sig * up
    act_ref[...] = act.astype(jnp.bfloat16)
    act_t_ref[...] = act.T.astype(jnp.bfloat16)


def mlp_bwd(gu, grad_act):
    tokens, ff = grad_act.shape
    rows = 128
    return pl.pallas_call(
        functools.partial(mlp_bwd_kernel, ff),
        grid=(tokens // rows,),
        in_specs=[pl.BlockSpec((rows, 2 * ff), lambda i: (i, 0)), pl.BlockSpec((rows, ff), lambda i: (i, 0))],
        out_specs=[pl.BlockSpec((rows, 2 * ff), lambda i: (i, 0)), pl.BlockSpec((rows, ff), lambda i: (i, 0)), pl.BlockSpec((ff, rows), lambda i: (0, i))],
        out_shape=[jax.ShapeDtypeStruct((tokens, 2 * ff), jnp.bfloat16), jax.ShapeDtypeStruct((tokens, ff), jnp.bfloat16), jax.ShapeDtypeStruct((ff, tokens), jnp.bfloat16)],
        cost_estimate=pl.CostEstimate(flops=16_000_000_000, bytes_accessed=50_000_000, transcendentals=3_200_000),
        name='mlp_bwd',
    )(gu, grad_act)


def solution(mesh):
    n_dev = mesh.shape[AXIS_NAME]
    n_chip = n_dev // 2
    pairs = [(i, i ^ 1) for i in range(n_dev)]
    same_core = [[2 * k + core for k in range(n_chip)] for core in range(2)]
    row_spec = P(AXIS_NAME, None)
    vec_spec = P(AXIS_NAME)
    full_spec = P(None)
    batch_spec = P(AXIS_NAME, None, None)
    weight_specs = (vec_spec, row_spec, row_spec, row_spec, full_spec, full_spec, row_spec, vec_spec, row_spec, row_spec, row_spec)

    def gather(shard):
        return lax.all_gather(shard, AXIS_NAME, tiled=True)

    def scatter_chips(part):
        return lax.psum_scatter(part, AXIS_NAME, scatter_dimension=0, tiled=True, axis_index_groups=same_core)

    def swap_core(part):
        return lax.ppermute(part, AXIS_NAME, pairs)

    def device_step(tokens, positions, table_shard, attn_norm, w_query, w_key, w_value, q_norm, k_norm, w_out, mlp_norm, w_gate, w_up, w_down, dy_out):
        me = lax.axis_index(AXIS_NAME)
        core = lax.rem(me, 2)
        batch, seq = tokens.shape
        rows_local, dim = table_shard.shape
        n_tok = batch * seq
        hd = q_norm.shape[0]
        kv_heads = w_key.shape[1] // hd
        n_rep = w_query.shape[1] // w_key.shape[1]
        ff = w_gate.shape[1]
        shard_rows = w_query.shape[0]

        def near_far(blocks, axis):
            return lax.dynamic_index_in_dim(blocks, core, axis, False), lax.dynamic_index_in_dim(blocks, 1 - core, axis, False)

        small = jnp.concatenate([tokens.reshape(-1).astype(jnp.float32), attn_norm.astype(jnp.float32), mlp_norm.astype(jnp.float32)])
        small = lax.all_gather(small, AXIS_NAME)
        attn_gain = small[:, n_tok:n_tok + shard_rows].reshape(1, dim)
        mlp_gain = small[:, n_tok + shard_rows:].reshape(1, dim)

        def group_columns(w):
            return w.reshape(w.shape[0], kv_heads, -1)

        qkv_shard = jnp.concatenate([group_columns(w_query), group_columns(w_key), group_columns(w_value)], axis=2).reshape(shard_rows, -1)
        gu_shard = jnp.concatenate([w_gate, w_up], axis=1)
        wqkv = gather(qkv_shard)
        small, gu_shard, _ = lax.optimization_barrier((small, gu_shard, qkv_shard))
        all_ids = small[:, :n_tok].astype(jnp.int32).reshape(n_chip, 2, batch, seq)

        def local_rows(ids, owner):
            local = ids - owner * rows_local
            return local, ((local >= 0) & (local < rows_local))[:, None]

        def pick(ids):
            local, _ = local_rows(ids, me)
            return jnp.take(table_shard, jnp.clip(local, 0, rows_local - 1), axis=0, mode='clip')

        seq_pad = -(-seq // 48) * 48

        def lookup(b):
            ids = jnp.pad(all_ids[:, :, b], ((0, 0), (0, 0), (0, seq_pad - seq)), constant_values=-1)
            near, far = near_far(ids, 1)
            near, far = near.reshape(-1), far.reshape(-1)
            recv = swap_core(pick(far))
            zero = jnp.zeros((), table_shard.dtype)
            merged = jnp.where(local_rows(near, me)[1], pick(near), jnp.where(local_rows(near, me + 1 - 2 * core)[1], recv, zero))
            return merged

        wo = gather(w_out)
        merged = []
        for b in range(batch):
            merged.append(lookup(b))
            merged[b], all_ids = lax.optimization_barrier((merged[b], all_ids))
        merged[-1], gu_shard, w_down = lax.optimization_barrier((merged[-1], gu_shard, w_down))
        x_emb = jnp.concatenate([scatter_chips(m)[:seq] for m in merged], axis=0)
        wgu = gather(gu_shard)
        wdown = gather(w_down)

        cos_t, sin_t = rope_tables(positions, hd)
        q_gain = q_norm.astype(jnp.float32)[None]
        k_gain = k_norm.astype(jnp.float32)[None]

        normed1, norm1_inv = norm_fwd(x_emb)
        attn_in = (normed1 * attn_gain).astype(jnp.bfloat16)
        qkv = dot_nn(attn_in, wqkv).astype(jnp.bfloat16)
        heads, *heads_rep = attn_fwd(qkv, cos_t, sin_t, q_gain, k_gain, batch, kv_heads, n_rep, hd)
        hidden = (x_emb.astype(jnp.float32) + dot_nn(heads, wo)).astype(jnp.bfloat16)
        normed2, norm2_inv = norm_fwd(hidden)
        mlp_in = (normed2 * mlp_gain).astype(jnp.bfloat16)
        gu = dot_nn(mlp_in, wgu)

        dy = dy_out.reshape(n_tok, dim)
        grad_act = dot_nt(dy, wdown)
        dgu, act, act_t = mlp_bwd(gu, grad_act)

        row_ids = jnp.arange(dim)

        def split_cores(a, block):
            pad = jnp.full((n_chip, 2, block - shard_rows), -1, row_ids.dtype)
            order = jnp.concatenate([row_ids.reshape(n_chip, 2, shard_rows), pad], axis=2)
            order = jnp.concatenate([part.reshape(-1) for part in near_far(order, 1)])
            select = (row_ids[:, None] == order[None, :]).astype(jnp.bfloat16)
            both = dot_nn(a, select).astype(jnp.bfloat16)
            return both[:, :n_chip * block], both[:, n_chip * block:]

        near2, far2 = split_cores(mlp_in, shard_rows)
        near_down, far_down = near_far(kdot_nn(act_t, dy).reshape(n_chip, 2, -1, dim), 1)
        part_down = near_down.reshape(-1, dim) + swap_core(far_down.reshape(-1, dim))
        far_gu, part_down, dgu = lax.optimization_barrier((dot_tn(far2, dgu), part_down, dgu))
        g_down = scatter_chips(part_down)
        recv_gu = swap_core(far_gu)
        grad_mlp_in = dot_nt(dgu, wgu)
        part_gu = dot_tn(near2, dgu) + recv_gu
        grad_mlp_norm = jnp.sum(grad_mlp_in * normed2, axis=0)
        grad_hidden = dy.astype(jnp.float32) + norm_bwd(grad_mlp_in, normed2, norm2_inv, mlp_gain)
        hidden_b = grad_hidden.astype(jnp.bfloat16)
        hidden_b, part_gu = lax.optimization_barrier((hidden_b, part_gu))
        g_gu = scatter_chips(part_gu)

        hidden_pad = jnp.pad(hidden_b, ((0, 0), (0, -dim % 384)))
        near_h = jnp.where(core == 0, heads_rep[0], heads_rep[1])
        far_h = jnp.where(core == 0, heads_rep[1], heads_rep[0])
        recv_out = swap_core(dot_tn(far_h, hidden_pad))
        grad_heads = dot_nt(hidden_b, wo).astype(jnp.bfloat16)
        part_out = dot_tn(near_h, hidden_pad) + recv_out
        grad_heads, part_out = lax.optimization_barrier((grad_heads, part_out))
        g_out = scatter_chips(part_out)[:, :dim]
        local_ids = (all_ids - me * rows_local).reshape(n_dev, batch, seq)
        slots = jnp.where((local_ids >= 0) & (local_ids < rows_local), local_ids, rows_local)
        grad_attn_norm, grad_q_norm, grad_k_norm = 0.0, 0.0, 0.0
        dqkv, all_rows = (), []
        for b in range(batch):
            rows = slice(b * seq, (b + 1) * seq)
            dqkv, dqg, dkg = attn_bwd(b, dqkv, qkv, grad_heads, cos_t, sin_t, q_gain, k_gain, batch, kv_heads, n_rep, hd)
            grad_attn_in = dot_nt(dqkv[rows], wqkv)
            grad_attn_norm += jnp.sum(grad_attn_in * normed1[rows], axis=0)
            grad_q_norm += jnp.sum(dqg, axis=0)
            grad_k_norm += jnp.sum(dkg, axis=0)
            grad_x = grad_hidden[rows] + norm_bwd(grad_attn_in, normed1[rows], norm1_inv[rows], attn_gain)
            grad_x, dqkv = lax.optimization_barrier((row_major(grad_x), dqkv))
            all_rows.append(gather(grad_x))
            dqkv = (dqkv,)
        dqkv, = dqkv
        near1, far1 = split_cores(attn_in, -(-shard_rows // 24) * 24)
        part_qkv = dot_tn(near1, dqkv) + swap_core(dot_tn(far1, dqkv))
        g_qkv = scatter_chips(part_qkv)[:shard_rows]
        layer_out = (hidden.astype(jnp.float32) + dot_nn(act, wdown)).astype(jnp.bfloat16)

        vec = jnp.concatenate([grad_attn_norm, grad_mlp_norm, grad_q_norm, grad_k_norm])
        vec, part_qkv, layer_out = lax.optimization_barrier((vec, part_qkv, layer_out))
        vec = jnp.sum(lax.all_gather(vec, AXIS_NAME), axis=0)
        g_attn_norm = lax.dynamic_slice_in_dim(vec[:dim], me * shard_rows, shard_rows)
        g_mlp_norm = lax.dynamic_slice_in_dim(vec[dim:2 * dim], me * shard_rows, shard_rows)
        g_q_norm = vec[2 * dim:2 * dim + hd]
        g_k_norm = vec[2 * dim + hd:]

        d_table = jnp.zeros((rows_local, dim), jnp.float32)
        for b in range(batch):
            d_table = d_table.at[slots[:, b].reshape(-1)].add(all_rows[b], mode='drop')

        g_qkv = g_qkv.reshape(shard_rows, kv_heads, n_rep + 2, hd)
        g_query = g_qkv[:, :, :n_rep].reshape(shard_rows, -1)
        g_key = g_qkv[:, :, n_rep].reshape(shard_rows, -1)
        g_value = g_qkv[:, :, n_rep + 1].reshape(shard_rows, -1)
        return (layer_out.reshape(dy_out.shape), d_table, g_attn_norm, g_query, g_key, g_value, g_q_norm, g_k_norm, g_out, g_mlp_norm, g_gu[:, :ff], g_gu[:, ff:], g_down)

    return jax.shard_map(device_step, mesh=mesh, in_specs=(row_spec, row_spec, row_spec) + weight_specs + (batch_spec,), out_specs=(batch_spec, row_spec) + weight_specs, check_vma=False)
```

```python
import functools
import math
import jax
import jax.numpy as jnp
from jax import lax
from jax.experimental import pallas as pl
from jax.experimental.layout import Layout, with_layout_constraint
from jax.experimental.pallas import tpu as pltpu
from jax.sharding import PartitionSpec as P

NORM_EPS = 1e-6
ROPE_THETA = 1.0e6
AXIS_NAME = 'fsdp'
NEG = -1e30


def split_rows(a):
    return a.reshape(2, a.shape[0] // 2, a.shape[1])


def kdot_nn(a, b):
    return lax.dot_general(a, b, (((1,), (0,)), ((), ())), preferred_element_type=jnp.float32)


def kdot_nt(a, b):
    return lax.dot_general(a, b, (((1,), (1,)), ((), ())), preferred_element_type=jnp.float32)


def dot_nn(a, b):
    return lax.dot_general(split_rows(a), b, (((2,), (0,)), ((), ())), preferred_element_type=jnp.float32).reshape(a.shape[0], -1)


def dot_nt(a, b):
    return lax.dot_general(split_rows(a), b, (((2,), (1,)), ((), ())), preferred_element_type=jnp.float32).reshape(a.shape[0], -1)


def dot_tn(a, b):
    return lax.dot_general(split_rows(a), split_rows(b), (((0, 1), (0, 1)), ((), ())), preferred_element_type=jnp.float32)


def row_major(a):
    return with_layout_constraint(a, Layout(major_to_minor=tuple(range(a.ndim))))


def norm_fwd(values):
    values_f = values.astype(jnp.float32)
    inv_rms = lax.rsqrt(jnp.mean(values_f * values_f, axis=-1, keepdims=True) + NORM_EPS)
    return values_f * inv_rms, inv_rms


def norm_bwd(grad_out, normed, inv_rms, gain_f):
    grad_normed = grad_out * gain_f
    mean_term = jnp.mean(grad_normed * normed, axis=-1, keepdims=True)
    return inv_rms * (grad_normed - normed * mean_term)


def rope_tables(positions, head_dim):
    half_dim = head_dim // 2
    inv_freq = jnp.exp(jnp.arange(half_dim, dtype=jnp.float32) * (-2.0 * math.log(ROPE_THETA) / head_dim))
    angles = positions.astype(jnp.float32).reshape(-1, 1) * inv_freq
    cos_t, sin_t = jnp.cos(angles), jnp.sin(angles)
    return jnp.concatenate([cos_t, cos_t], axis=-1), jnp.concatenate([-sin_t, sin_t], axis=-1)


def rope(values, cos_t, sin_t):
    return values * cos_t + pltpu.roll(values, values.shape[-1] // 2, 1) * sin_t


def attn_fwd_kernel(n_rep, hd, chunk, qkv_ref, cos_ref, sin_ref, qg_ref, kg_ref, out_ref, *rep_refs):
    seq = qkv_ref.shape[0]
    scale = hd ** -0.5
    cos_t, sin_t = cos_ref[...], sin_ref[...]
    k_n, _ = norm_fwd(qkv_ref[:, n_rep * hd:(n_rep + 1) * hd])
    k_rot = rope(k_n * kg_ref[...], cos_t, sin_t).astype(jnp.bfloat16)
    v_t = qkv_ref[:, (n_rep + 1) * hd:(n_rep + 2) * hd].astype(jnp.float32).T.astype(jnp.bfloat16)
    for rep in range(n_rep):
        q_n, _ = norm_fwd(qkv_ref[:, rep * hd:(rep + 1) * hd])
        q_rot = rope(q_n * qg_ref[...], cos_t, sin_t).astype(jnp.bfloat16)
        for lo in range(0, seq, chunk):
            end = lo + chunk
            s = kdot_nt(k_rot[:end], q_rot[lo:end]) * scale
            keys = lax.broadcasted_iota(jnp.int32, s.shape, 0)
            qpos = lax.broadcasted_iota(jnp.int32, s.shape, 1) + lo
            s = jnp.where(qpos >= keys, s, NEG)
            e = jnp.exp(s - jnp.max(s, axis=0, keepdims=True))
            p = e * (1.0 / jnp.sum(e, axis=0, keepdims=True))
            o = kdot_nn(v_t[:, :end], p.astype(jnp.bfloat16)).T
            out_ref[lo:end, rep * hd:(rep + 1) * hd] = o.astype(jnp.bfloat16)
            rep_refs[rep][lo:end] = o.astype(jnp.bfloat16)


def attn_fwd(qkv, cos_t, sin_t, q_gain, k_gain, batch, kv_heads, n_rep, hd):
    tokens, width = qkv.shape
    seq = tokens // batch
    gw = width // kv_heads
    return pl.pallas_call(
        functools.partial(attn_fwd_kernel, n_rep, hd, seq // 2),
        grid=(batch, kv_heads),
        in_specs=[pl.BlockSpec((seq, gw), lambda b, g: (b, g)),
                  pl.BlockSpec((seq, hd), lambda b, g: (b, 0)),
                  pl.BlockSpec((seq, hd), lambda b, g: (b, 0)),
                  pl.BlockSpec((1, hd), lambda b, g: (0, 0)),
                  pl.BlockSpec((1, hd), lambda b, g: (0, 0))],
        out_specs=[pl.BlockSpec((seq, n_rep * hd), lambda b, g: (b, g))] + [pl.BlockSpec((seq, hd), lambda b, g: (b, g))] * n_rep,
        out_shape=[jax.ShapeDtypeStruct((tokens, kv_heads * n_rep * hd), jnp.bfloat16)] + [jax.ShapeDtypeStruct((tokens, kv_heads * hd), jnp.bfloat16)] * n_rep,
        cost_estimate=pl.CostEstimate(flops=25_000_000_000, bytes_accessed=14_000_000, transcendentals=8_400_000),
        name='attn_fwd',
    )(qkv, cos_t, sin_t, q_gain, k_gain)


def attn_bwd_kernel(n_rep, hd, chunk, n_alias, qkv_ref, do_ref, cos_ref, sin_ref, qg_ref, kg_ref, *rest):
    dqkv_ref, dqg_ref, dkg_ref, dk_acc, dv_acc = rest[n_alias:]
    seq = qkv_ref.shape[0]
    scale = hd ** -0.5
    cos_t, sin_t = cos_ref[...], sin_ref[...]
    qg, kg = qg_ref[...], kg_ref[...]

    @pl.when(pl.program_id(0) == 0)
    def _():
        dqg_ref[...] = jnp.zeros_like(dqg_ref)
        dkg_ref[...] = jnp.zeros_like(dkg_ref)

    k_n, k_inv = norm_fwd(qkv_ref[:, n_rep * hd:(n_rep + 1) * hd])
    k_rot_f = rope(k_n * kg, cos_t, sin_t)
    k_rot = k_rot_f.astype(jnp.bfloat16)
    k_rot_t = k_rot_f.T.astype(jnp.bfloat16)
    v_raw = qkv_ref[:, (n_rep + 1) * hd:(n_rep + 2) * hd]
    dk_acc[...] = jnp.zeros_like(dk_acc)
    dv_acc[...] = jnp.zeros_like(dv_acc)
    for rep in range(n_rep):
        q_n, q_inv = norm_fwd(qkv_ref[:, rep * hd:(rep + 1) * hd])
        q_rot = rope(q_n * qg, cos_t, sin_t).astype(jnp.bfloat16)
        dq_parts = []
        for lo in range(0, seq, chunk):
            end = lo + chunk
            q_c = q_rot[lo:end]
            do_c = do_ref[lo:end, rep * hd:(rep + 1) * hd]
            s = kdot_nt(k_rot[:end], q_c) * scale
            keys = lax.broadcasted_iota(jnp.int32, s.shape, 0)
            qpos = lax.broadcasted_iota(jnp.int32, s.shape, 1) + lo
            s = jnp.where(qpos >= keys, s, NEG)
            e = jnp.exp(s - jnp.max(s, axis=0, keepdims=True))
            p = e * (1.0 / jnp.sum(e, axis=0, keepdims=True))
            dv_acc[:end] += kdot_nn(p.astype(jnp.bfloat16), do_c)
            dp = kdot_nt(v_raw[:end], do_c)
            delta = jnp.sum(dp * p, axis=0, keepdims=True)
            ds = (p * (dp - delta) * scale).astype(jnp.bfloat16)
            dk_acc[:end] += kdot_nn(ds, q_c)
            dq_parts.append(kdot_nn(k_rot_t[:, :end], ds).T)
        dq = jnp.concatenate(dq_parts, axis=0)
        dqt = dq * cos_t - pltpu.roll(dq, hd // 2, 1) * sin_t
        dqg_ref[...] += jnp.sum((dqt * q_n).reshape(seq // 8, 8, hd), axis=0)
        dqkv_ref[:, rep * hd:(rep + 1) * hd] = norm_bwd(dqt, q_n, q_inv, qg).astype(jnp.bfloat16)
    dk = dk_acc[...]
    dkt = dk * cos_t - pltpu.roll(dk, hd // 2, 1) * sin_t
    dkg_ref[...] += jnp.sum((dkt * k_n).reshape(seq // 8, 8, hd), axis=0)
    dqkv_ref[:, n_rep * hd:(n_rep + 1) * hd] = norm_bwd(dkt, k_n, k_inv, kg).astype(jnp.bfloat16)
    dqkv_ref[:, (n_rep + 1) * hd:(n_rep + 2) * hd] = dv_acc[...].astype(jnp.bfloat16)


def attn_bwd(b, prev, qkv, do, cos_t, sin_t, q_gain, k_gain, batch, kv_heads, n_rep, hd):
    tokens, width = qkv.shape
    seq = tokens // batch
    gw = width // kv_heads
    return pl.pallas_call(
        functools.partial(attn_bwd_kernel, n_rep, hd, seq // 2, len(prev)),
        grid=(kv_heads,),
        in_specs=[pl.BlockSpec((seq, gw), lambda g: (b, g)),
                  pl.BlockSpec((seq, n_rep * hd), lambda g: (b, g)),
                  pl.BlockSpec((seq, hd), lambda g: (b, 0)),
                  pl.BlockSpec((seq, hd), lambda g: (b, 0)),
                  pl.BlockSpec((1, hd), lambda g: (0, 0)),
                  pl.BlockSpec((1, hd), lambda g: (0, 0))] + [pl.BlockSpec(memory_space=pl.ANY)] * len(prev),
        out_specs=[pl.BlockSpec((seq, gw), lambda g: (b, g)),
                   pl.BlockSpec((8, hd), lambda g: (0, 0)),
                   pl.BlockSpec((8, hd), lambda g: (0, 0))],
        out_shape=[jax.ShapeDtypeStruct((tokens, width), jnp.bfloat16),
                   jax.ShapeDtypeStruct((8, hd), jnp.float32),
                   jax.ShapeDtypeStruct((8, hd), jnp.float32)],
        input_output_aliases={6: 0} if prev else {},
        scratch_shapes=[pltpu.VMEM((seq, hd), jnp.float32), pltpu.VMEM((seq, hd), jnp.float32)],
        cost_estimate=pl.CostEstimate(flops=25_000_000_000, bytes_accessed=14_000_000, transcendentals=4_200_000),
        name='attn_bwd',
    )(qkv, do, cos_t, sin_t, q_gain, k_gain, *prev)


def mlp_act_kernel(ff, n_chip, core_ref, gu_ref, act_ref, act_t_ref):
    gate, up = gu_ref[:, :ff], gu_ref[:, ff:]
    act = gate * jax.nn.sigmoid(gate) * up
    act_ref[...] = act.astype(jnp.bfloat16)
    act_t = act.T.astype(jnp.bfloat16)
    block = ff // (2 * n_chip)
    for i in range(2 * n_chip):
        act_t_ref[lax.bitwise_xor(core_ref[0], i % 2), i // 2] = act_t[i * block:(i + 1) * block]


def mlp_act(gu, core, n_chip):
    tokens, ff = gu.shape[0], gu.shape[1] // 2
    rows = 128
    return pl.pallas_call(
        functools.partial(mlp_act_kernel, ff, n_chip),
        grid=(tokens // rows,),
        in_specs=[pl.BlockSpec(memory_space=pltpu.SMEM), pl.BlockSpec((rows, 2 * ff), lambda i: (i, 0))],
        out_specs=[pl.BlockSpec((rows, ff), lambda i: (i, 0)), pl.BlockSpec((2, n_chip, ff // (2 * n_chip), rows), lambda i: (0, 0, 0, i))],
        out_shape=[jax.ShapeDtypeStruct((tokens, ff), jnp.bfloat16), jax.ShapeDtypeStruct((2, n_chip, ff // (2 * n_chip), tokens), jnp.bfloat16)],
        cost_estimate=pl.CostEstimate(flops=12_000_000_000, bytes_accessed=38_000_000, transcendentals=3_200_000),
        name='mlp_act',
    )(core.reshape(1), gu)


def mlp_bwd_kernel(ff, gu_ref, ga_ref, out_ref):
    gate, up, grad_act = gu_ref[:, :ff], gu_ref[:, ff:], ga_ref[...]
    sig = jax.nn.sigmoid(gate)
    out_ref[:, :ff] = (grad_act * up * sig * (1.0 + gate * (1.0 - sig))).astype(jnp.bfloat16)
    out_ref[:, ff:] = (grad_act * gate * sig).astype(jnp.bfloat16)


def mlp_bwd(gu, grad_act):
    tokens, ff = grad_act.shape
    rows = 128
    return pl.pallas_call(
        functools.partial(mlp_bwd_kernel, ff),
        grid=(tokens // rows,),
        in_specs=[pl.BlockSpec((rows, 2 * ff), lambda i: (i, 0)), pl.BlockSpec((rows, ff), lambda i: (i, 0))],
        out_specs=pl.BlockSpec((rows, 2 * ff), lambda i: (i, 0)),
        out_shape=jax.ShapeDtypeStruct((tokens, 2 * ff), jnp.bfloat16),
        cost_estimate=pl.CostEstimate(flops=16_000_000_000, bytes_accessed=50_000_000, transcendentals=3_200_000),
        name='mlp_bwd',
    )(gu, grad_act)


def solution(mesh):
    n_dev = mesh.shape[AXIS_NAME]
    n_chip = n_dev // 2
    pairs = [(i, i ^ 1) for i in range(n_dev)]
    same_core = [[2 * k + core for k in range(n_chip)] for core in range(2)]
    row_spec = P(AXIS_NAME, None)
    vec_spec = P(AXIS_NAME)
    full_spec = P(None)
    batch_spec = P(AXIS_NAME, None, None)
    weight_specs = (vec_spec, row_spec, row_spec, row_spec, full_spec, full_spec, row_spec, vec_spec, row_spec, row_spec, row_spec)

    def gather(shard):
        return lax.all_gather(shard, AXIS_NAME, tiled=True)

    def scatter_chips(part):
        return lax.psum_scatter(part, AXIS_NAME, scatter_dimension=0, tiled=True, axis_index_groups=same_core)

    def swap_core(part):
        return lax.ppermute(part, AXIS_NAME, pairs)

    def device_step(tokens, positions, table_shard, attn_norm, w_query, w_key, w_value, q_norm, k_norm, w_out, mlp_norm, w_gate, w_up, w_down, dy_out):
        me = lax.axis_index(AXIS_NAME)
        core = lax.rem(me, 2)
        batch, seq = tokens.shape
        rows_local, dim = table_shard.shape
        n_tok = batch * seq
        hd = q_norm.shape[0]
        kv_heads = w_key.shape[1] // hd
        n_rep = w_query.shape[1] // w_key.shape[1]
        ff = w_gate.shape[1]
        shard_rows = w_query.shape[0]

        def near_far(blocks, axis):
            return lax.dynamic_index_in_dim(blocks, core, axis, False), lax.dynamic_index_in_dim(blocks, 1 - core, axis, False)

        small = jnp.concatenate([tokens.reshape(-1).astype(jnp.float32), attn_norm.astype(jnp.float32), mlp_norm.astype(jnp.float32)])
        small = lax.all_gather(small, AXIS_NAME)
        attn_gain = small[:, n_tok:n_tok + shard_rows].reshape(1, dim)
        mlp_gain = small[:, n_tok + shard_rows:].reshape(1, dim)

        def group_columns(w):
            return w.reshape(w.shape[0], kv_heads, -1)

        qkv_shard = jnp.concatenate([group_columns(w_query), group_columns(w_key), group_columns(w_value)], axis=2).reshape(shard_rows, -1)
        gu_shard = jnp.concatenate([w_gate, w_up], axis=1)
        wqkv = gather(qkv_shard)
        small, gu_shard, _ = lax.optimization_barrier((small, gu_shard, qkv_shard))
        all_ids = small[:, :n_tok].astype(jnp.int32).reshape(n_chip, 2, batch, seq)

        def local_rows(ids, owner):
            local = ids - owner * rows_local
            return local, ((local >= 0) & (local < rows_local))[:, None]

        def pick(ids):
            local, _ = local_rows(ids, me)
            return jnp.take(table_shard, jnp.clip(local, 0, rows_local - 1), axis=0, mode='clip')

        seq_pad = -(-seq // 48) * 48

        def lookup(b):
            ids = jnp.pad(all_ids[:, :, b], ((0, 0), (0, 0), (0, seq_pad - seq)), constant_values=-1)
            near, far = near_far(ids, 1)
            near, far = near.reshape(-1), far.reshape(-1)
            near_rows, far_rows = pick(near), pick(far)
            recv = swap_core(far_rows)
            zero = jnp.zeros((), table_shard.dtype)
            merged = jnp.where(local_rows(near, me)[1], near_rows, jnp.where(local_rows(near, me + 1 - 2 * core)[1], recv, zero))
            return merged

        wo = gather(w_out)
        merged = []
        for b in range(batch):
            merged.append(lookup(b))
            merged[b], all_ids = lax.optimization_barrier((merged[b], all_ids))
        merged[-1], gu_shard, w_down = lax.optimization_barrier((merged[-1], gu_shard, w_down))
        x_emb = jnp.concatenate([scatter_chips(m)[:seq] for m in merged], axis=0)
        wgu = gather(gu_shard)
        wdown = gather(w_down)

        cos_t, sin_t = rope_tables(positions, hd)
        q_gain = q_norm.astype(jnp.float32)[None]
        k_gain = k_norm.astype(jnp.float32)[None]

        normed1, norm1_inv = norm_fwd(x_emb)
        attn_in = (normed1 * attn_gain).astype(jnp.bfloat16)
        qkv = dot_nn(attn_in, wqkv).astype(jnp.bfloat16)
        heads, *heads_rep = attn_fwd(qkv, cos_t, sin_t, q_gain, k_gain, batch, kv_heads, n_rep, hd)
        hidden = (x_emb.astype(jnp.float32) + dot_nn(heads, wo)).astype(jnp.bfloat16)
        normed2, norm2_inv = norm_fwd(hidden)
        mlp_in = (normed2 * mlp_gain).astype(jnp.bfloat16)
        gu = dot_nn(mlp_in, wgu)

        act, act_t = mlp_act(gu, core, n_chip)

        dy = dy_out.reshape(n_tok, dim)
        part_down = kdot_nn(act_t[0].reshape(-1, n_tok), dy) + swap_core(kdot_nn(act_t[1].reshape(-1, n_tok), dy))
        dy_b, part_down = lax.optimization_barrier((dy, part_down))
        g_down = scatter_chips(part_down)
        grad_act = dot_nt(dy_b, wdown)
        dgu = mlp_bwd(gu, grad_act)

        row_ids = jnp.arange(dim)

        def split_cores(a, block):
            pad = jnp.full((n_chip, 2, block - shard_rows), -1, row_ids.dtype)
            order = jnp.concatenate([row_ids.reshape(n_chip, 2, shard_rows), pad], axis=2)
            order = jnp.concatenate([part.reshape(-1) for part in near_far(order, 1)])
            select = (row_ids[:, None] == order[None, :]).astype(jnp.bfloat16)
            both = dot_nn(a, select).astype(jnp.bfloat16)
            return both[:, :n_chip * block], both[:, n_chip * block:]

        near2, far2 = split_cores(mlp_in, shard_rows)
        far_gu, dgu = lax.optimization_barrier((dot_tn(far2, dgu), dgu))
        recv_gu = swap_core(far_gu)
        grad_mlp_in = dot_nt(dgu, wgu)
        part_gu = dot_tn(near2, dgu) + recv_gu
        grad_mlp_norm = jnp.sum(grad_mlp_in * normed2, axis=0)
        grad_hidden = dy.astype(jnp.float32) + norm_bwd(grad_mlp_in, normed2, norm2_inv, mlp_gain)
        hidden_b = grad_hidden.astype(jnp.bfloat16)
        hidden_b, part_gu = lax.optimization_barrier((hidden_b, part_gu))
        g_gu = scatter_chips(part_gu)

        hidden_pad = jnp.pad(hidden_b, ((0, 0), (0, -dim % 384)))
        near_h = jnp.where(core == 0, heads_rep[0], heads_rep[1])
        far_h = jnp.where(core == 0, heads_rep[1], heads_rep[0])
        recv_out = swap_core(dot_tn(far_h, hidden_pad))
        grad_heads = dot_nt(hidden_b, wo).astype(jnp.bfloat16)
        part_out = dot_tn(near_h, hidden_pad) + recv_out
        g_out = scatter_chips(part_out)[:, :dim]
        local_ids = (all_ids - me * rows_local).reshape(n_dev, batch, seq)
        slots = jnp.where((local_ids >= 0) & (local_ids < rows_local), local_ids, rows_local)
        grad_attn_norm, grad_q_norm, grad_k_norm = 0.0, 0.0, 0.0
        dqkv, all_rows = (), []
        for b in range(batch):
            rows = slice(b * seq, (b + 1) * seq)
            dqkv, dqg, dkg = attn_bwd(b, dqkv, qkv, grad_heads, cos_t, sin_t, q_gain, k_gain, batch, kv_heads, n_rep, hd)
            grad_attn_in = dot_nt(dqkv[rows], wqkv)
            grad_attn_norm += jnp.sum(grad_attn_in * normed1[rows], axis=0)
            grad_q_norm += jnp.sum(dqg, axis=0)
            grad_k_norm += jnp.sum(dkg, axis=0)
            grad_x = grad_hidden[rows] + norm_bwd(grad_attn_in, normed1[rows], norm1_inv[rows], attn_gain)
            grad_x, dqkv = lax.optimization_barrier((row_major(grad_x), dqkv))
            all_rows.append(gather(grad_x))
            dqkv = (dqkv,)
        dqkv, = dqkv
        near1, far1 = split_cores(attn_in, -(-shard_rows // 24) * 24)
        far_qkv = dot_tn(far1, dqkv)
        part_qkv = dot_tn(near1, dqkv) + swap_core(far_qkv)
        g_qkv = scatter_chips(part_qkv)[:shard_rows]
        layer_out = (hidden.astype(jnp.float32) + dot_nn(act, wdown)).astype(jnp.bfloat16)

        vec = jnp.concatenate([grad_attn_norm, grad_mlp_norm, grad_q_norm, grad_k_norm])
        vec, part_qkv, layer_out = lax.optimization_barrier((vec, part_qkv, layer_out))
        vec = jnp.sum(lax.all_gather(vec, AXIS_NAME), axis=0)
        g_attn_norm = lax.dynamic_slice_in_dim(vec[:dim], me * shard_rows, shard_rows)
        g_mlp_norm = lax.dynamic_slice_in_dim(vec[dim:2 * dim], me * shard_rows, shard_rows)
        g_q_norm = vec[2 * dim:2 * dim + hd]
        g_k_norm = vec[2 * dim + hd:]

        d_table = jnp.zeros((rows_local, dim), jnp.float32)
        for b in range(batch):
            d_table = d_table.at[slots[:, b].reshape(-1)].add(all_rows[b], mode='drop')

        g_qkv = g_qkv.reshape(shard_rows, kv_heads, n_rep + 2, hd)
        g_query = g_qkv[:, :, :n_rep].reshape(shard_rows, -1)
        g_key = g_qkv[:, :, n_rep].reshape(shard_rows, -1)
        g_value = g_qkv[:, :, n_rep + 1].reshape(shard_rows, -1)
        return (layer_out.reshape(dy_out.shape), d_table, g_attn_norm, g_query, g_key, g_value, g_q_norm, g_k_norm, g_out, g_mlp_norm, g_gu[:, :ff], g_gu[:, ff:], g_down)

    return jax.shard_map(device_step, mesh=mesh, in_specs=(row_spec, row_spec, row_spec) + weight_specs + (batch_spec,), out_specs=(batch_spec, row_spec) + weight_specs, check_vma=False)
```

```python
import functools
import math
import jax
import jax.numpy as jnp
from jax import lax
from jax.experimental import pallas as pl
from jax.experimental.layout import Layout, with_layout_constraint
from jax.experimental.pallas import tpu as pltpu
from jax.sharding import PartitionSpec as P

NORM_EPS = 1e-6
ROPE_THETA = 1.0e6
AXIS_NAME = 'fsdp'
NEG = -1e30


def split_rows(a):
    return a.reshape(2, a.shape[0] // 2, a.shape[1])


def kdot_nn(a, b):
    return lax.dot_general(a, b, (((1,), (0,)), ((), ())), preferred_element_type=jnp.float32)


def kdot_nt(a, b):
    return lax.dot_general(a, b, (((1,), (1,)), ((), ())), preferred_element_type=jnp.float32)


def dot_nn(a, b):
    return lax.dot_general(split_rows(a), b, (((2,), (0,)), ((), ())), preferred_element_type=jnp.float32).reshape(a.shape[0], -1)


def dot_nt(a, b):
    return lax.dot_general(split_rows(a), b, (((2,), (1,)), ((), ())), preferred_element_type=jnp.float32).reshape(a.shape[0], -1)


def dot_tn(a, b):
    return lax.dot_general(split_rows(a), split_rows(b), (((0, 1), (0, 1)), ((), ())), preferred_element_type=jnp.float32)


def row_major(a):
    return with_layout_constraint(a, Layout(major_to_minor=tuple(range(a.ndim))))


def norm_fwd(values):
    values_f = values.astype(jnp.float32)
    inv_rms = lax.rsqrt(jnp.mean(values_f * values_f, axis=-1, keepdims=True) + NORM_EPS)
    return values_f * inv_rms, inv_rms


def norm_bwd(grad_out, normed, inv_rms, gain_f):
    grad_normed = grad_out * gain_f
    mean_term = jnp.mean(grad_normed * normed, axis=-1, keepdims=True)
    return inv_rms * (grad_normed - normed * mean_term)


def rope_tables(positions, head_dim):
    half_dim = head_dim // 2
    inv_freq = jnp.exp(jnp.arange(half_dim, dtype=jnp.float32) * (-2.0 * math.log(ROPE_THETA) / head_dim))
    angles = positions.astype(jnp.float32).reshape(-1, 1) * inv_freq
    cos_t, sin_t = jnp.cos(angles), jnp.sin(angles)
    return jnp.concatenate([cos_t, cos_t], axis=-1), jnp.concatenate([-sin_t, sin_t], axis=-1)


def rope(values, cos_t, sin_t):
    return values * cos_t + pltpu.roll(values, values.shape[-1] // 2, 1) * sin_t


def attn_fwd_kernel(n_rep, hd, chunk, n_alias, qkv_ref, cos_ref, sin_ref, qg_ref, kg_ref, *rest):
    out_ref, *rep_refs = rest[n_alias:]
    seq = qkv_ref.shape[0]
    scale = hd ** -0.5
    cos_t, sin_t = cos_ref[...], sin_ref[...]
    k_n, _ = norm_fwd(qkv_ref[:, n_rep * hd:(n_rep + 1) * hd])
    k_rot = rope(k_n * kg_ref[...], cos_t, sin_t).astype(jnp.bfloat16)
    v_t = qkv_ref[:, (n_rep + 1) * hd:(n_rep + 2) * hd].astype(jnp.float32).T.astype(jnp.bfloat16)
    for rep in range(n_rep):
        q_n, _ = norm_fwd(qkv_ref[:, rep * hd:(rep + 1) * hd])
        q_rot = rope(q_n * qg_ref[...], cos_t, sin_t).astype(jnp.bfloat16)
        for lo in range(0, seq, chunk):
            end = lo + chunk
            s = kdot_nt(k_rot[:end], q_rot[lo:end]) * scale
            keys = lax.broadcasted_iota(jnp.int32, s.shape, 0)
            qpos = lax.broadcasted_iota(jnp.int32, s.shape, 1) + lo
            s = jnp.where(qpos >= keys, s, NEG)
            e = jnp.exp(s - jnp.max(s, axis=0, keepdims=True))
            p = e * (1.0 / jnp.sum(e, axis=0, keepdims=True))
            o = kdot_nn(v_t[:, :end], p.astype(jnp.bfloat16)).T
            out_ref[lo:end, rep * hd:(rep + 1) * hd] = o.astype(jnp.bfloat16)
            rep_refs[rep][lo:end] = o.astype(jnp.bfloat16)


def attn_fwd(b, prev, qkv, cos_t, sin_t, q_gain, k_gain, batch, kv_heads, n_rep, hd):
    seq, width = qkv.shape
    gw = width // kv_heads
    return pl.pallas_call(
        functools.partial(attn_fwd_kernel, n_rep, hd, seq // 2, len(prev)),
        grid=(kv_heads,),
        in_specs=[pl.BlockSpec((seq, gw), lambda g: (0, g)),
                  pl.BlockSpec((seq, hd), lambda g: (b, 0)),
                  pl.BlockSpec((seq, hd), lambda g: (b, 0)),
                  pl.BlockSpec((1, hd), lambda g: (0, 0)),
                  pl.BlockSpec((1, hd), lambda g: (0, 0))] + [pl.BlockSpec(memory_space=pl.ANY)] * len(prev),
        out_specs=[pl.BlockSpec((seq, n_rep * hd), lambda g: (b, g))] + [pl.BlockSpec((seq, hd), lambda g: (b, g))] * n_rep,
        out_shape=[jax.ShapeDtypeStruct((seq * batch, kv_heads * n_rep * hd), jnp.bfloat16)] + [jax.ShapeDtypeStruct((seq * batch, kv_heads * hd), jnp.bfloat16)] * n_rep,
        input_output_aliases={5 + n: n for n in range(len(prev))},
        cost_estimate=pl.CostEstimate(flops=12_000_000_000, bytes_accessed=8_000_000, transcendentals=4_200_000),
        name='attn_fwd',
    )(qkv, cos_t, sin_t, q_gain, k_gain, *prev)


def attn_bwd_kernel(n_rep, hd, chunk, n_alias, qkv_ref, do_ref, cos_ref, sin_ref, qg_ref, kg_ref, *rest):
    dqkv_ref, dqg_ref, dkg_ref, dk_acc, dv_acc = rest[n_alias:]
    seq = qkv_ref.shape[0]
    scale = hd ** -0.5
    cos_t, sin_t = cos_ref[...], sin_ref[...]
    qg, kg = qg_ref[...], kg_ref[...]

    @pl.when(pl.program_id(0) == 0)
    def _():
        dqg_ref[...] = jnp.zeros_like(dqg_ref)
        dkg_ref[...] = jnp.zeros_like(dkg_ref)

    k_n, k_inv = norm_fwd(qkv_ref[:, n_rep * hd:(n_rep + 1) * hd])
    k_rot_f = rope(k_n * kg, cos_t, sin_t)
    k_rot = k_rot_f.astype(jnp.bfloat16)
    k_rot_t = k_rot_f.T.astype(jnp.bfloat16)
    v_raw = qkv_ref[:, (n_rep + 1) * hd:(n_rep + 2) * hd]
    dk_acc[...] = jnp.zeros_like(dk_acc)
    dv_acc[...] = jnp.zeros_like(dv_acc)
    for rep in range(n_rep):
        q_n, q_inv = norm_fwd(qkv_ref[:, rep * hd:(rep + 1) * hd])
        q_rot = rope(q_n * qg, cos_t, sin_t).astype(jnp.bfloat16)
        dq_parts = []
        for lo in range(0, seq, chunk):
            end = lo + chunk
            q_c = q_rot[lo:end]
            do_c = do_ref[lo:end, rep * hd:(rep + 1) * hd]
            s = kdot_nt(k_rot[:end], q_c) * scale
            keys = lax.broadcasted_iota(jnp.int32, s.shape, 0)
            qpos = lax.broadcasted_iota(jnp.int32, s.shape, 1) + lo
            s = jnp.where(qpos >= keys, s, NEG)
            e = jnp.exp(s - jnp.max(s, axis=0, keepdims=True))
            p = e * (1.0 / jnp.sum(e, axis=0, keepdims=True))
            dv_acc[:end] += kdot_nn(p.astype(jnp.bfloat16), do_c)
            dp = kdot_nt(v_raw[:end], do_c)
            delta = jnp.sum(dp * p, axis=0, keepdims=True)
            ds = (p * (dp - delta) * scale).astype(jnp.bfloat16)
            dk_acc[:end] += kdot_nn(ds, q_c)
            dq_parts.append(kdot_nn(k_rot_t[:, :end], ds).T)
        dq = jnp.concatenate(dq_parts, axis=0)
        dqt = dq * cos_t - pltpu.roll(dq, hd // 2, 1) * sin_t
        dqg_ref[...] += jnp.sum((dqt * q_n).reshape(seq // 8, 8, hd), axis=0)
        dqkv_ref[:, rep * hd:(rep + 1) * hd] = norm_bwd(dqt, q_n, q_inv, qg).astype(jnp.bfloat16)
    dk = dk_acc[...]
    dkt = dk * cos_t - pltpu.roll(dk, hd // 2, 1) * sin_t
    dkg_ref[...] += jnp.sum((dkt * k_n).reshape(seq // 8, 8, hd), axis=0)
    dqkv_ref[:, n_rep * hd:(n_rep + 1) * hd] = norm_bwd(dkt, k_n, k_inv, kg).astype(jnp.bfloat16)
    dqkv_ref[:, (n_rep + 1) * hd:(n_rep + 2) * hd] = dv_acc[...].astype(jnp.bfloat16)


def attn_bwd(b, prev, qkv, do, cos_t, sin_t, q_gain, k_gain, batch, kv_heads, n_rep, hd):
    seq, width = qkv.shape
    tokens = seq * batch
    gw = width // kv_heads
    return pl.pallas_call(
        functools.partial(attn_bwd_kernel, n_rep, hd, seq // 2, len(prev)),
        grid=(kv_heads,),
        in_specs=[pl.BlockSpec((seq, gw), lambda g: (0, g)),
                  pl.BlockSpec((seq, n_rep * hd), lambda g: (b, g)),
                  pl.BlockSpec((seq, hd), lambda g: (b, 0)),
                  pl.BlockSpec((seq, hd), lambda g: (b, 0)),
                  pl.BlockSpec((1, hd), lambda g: (0, 0)),
                  pl.BlockSpec((1, hd), lambda g: (0, 0))] + [pl.BlockSpec(memory_space=pl.ANY)] * len(prev),
        out_specs=[pl.BlockSpec((seq, gw), lambda g: (b, g)),
                   pl.BlockSpec((8, hd), lambda g: (0, 0)),
                   pl.BlockSpec((8, hd), lambda g: (0, 0))],
        out_shape=[jax.ShapeDtypeStruct((tokens, width), jnp.bfloat16),
                   jax.ShapeDtypeStruct((8, hd), jnp.float32),
                   jax.ShapeDtypeStruct((8, hd), jnp.float32)],
        input_output_aliases={6: 0} if prev else {},
        scratch_shapes=[pltpu.VMEM((seq, hd), jnp.float32), pltpu.VMEM((seq, hd), jnp.float32)],
        cost_estimate=pl.CostEstimate(flops=25_000_000_000, bytes_accessed=14_000_000, transcendentals=4_200_000),
        name='attn_bwd',
    )(qkv, do, cos_t, sin_t, q_gain, k_gain, *prev)


def mlp_act_kernel(ff, n_chip, core_ref, gu_ref, act_ref, near_ref, far_ref):
    gate, up = gu_ref[:, :ff], gu_ref[:, ff:]
    act = gate * jax.nn.sigmoid(gate) * up
    act_ref[...] = act.astype(jnp.bfloat16)
    act_t = act.T.astype(jnp.bfloat16)
    block = ff // (2 * n_chip)
    first = core_ref[0] == 0
    for k in range(n_chip):
        even, odd = act_t[2 * k * block:(2 * k + 1) * block], act_t[(2 * k + 1) * block:(2 * k + 2) * block]
        near_ref[k * block:(k + 1) * block] = jnp.where(first, even, odd)
        far_ref[k * block:(k + 1) * block] = jnp.where(first, odd, even)


def mlp_act(gu, core, n_chip):
    tokens, ff = gu.shape[0], gu.shape[1] // 2
    rows = 128
    return pl.pallas_call(
        functools.partial(mlp_act_kernel, ff, n_chip),
        grid=(tokens // rows,),
        in_specs=[pl.BlockSpec(memory_space=pltpu.SMEM), pl.BlockSpec((rows, 2 * ff), lambda i: (i, 0))],
        out_specs=[pl.BlockSpec((rows, ff), lambda i: (i, 0)), pl.BlockSpec((ff // 2, rows), lambda i: (0, i)), pl.BlockSpec((ff // 2, rows), lambda i: (0, i))],
        out_shape=[jax.ShapeDtypeStruct((tokens, ff), jnp.bfloat16), jax.ShapeDtypeStruct((ff // 2, tokens), jnp.bfloat16), jax.ShapeDtypeStruct((ff // 2, tokens), jnp.bfloat16)],
        cost_estimate=pl.CostEstimate(flops=12_000_000_000, bytes_accessed=38_000_000, transcendentals=3_200_000),
        name='mlp_act',
    )(core.reshape(1), gu)


def mlp_bwd_kernel(ff, gu_ref, ga_ref, out_ref):
    gate, up, grad_act = gu_ref[:, :ff], gu_ref[:, ff:], ga_ref[...]
    sig = jax.nn.sigmoid(gate)
    out_ref[:, :ff] = (grad_act * up * sig * (1.0 + gate * (1.0 - sig))).astype(jnp.bfloat16)
    out_ref[:, ff:] = (grad_act * gate * sig).astype(jnp.bfloat16)


def mlp_bwd(gu, grad_act):
    tokens, ff = grad_act.shape
    rows = 128
    return pl.pallas_call(
        functools.partial(mlp_bwd_kernel, ff),
        grid=(tokens // rows,),
        in_specs=[pl.BlockSpec((rows, 2 * ff), lambda i: (i, 0)), pl.BlockSpec((rows, ff), lambda i: (i, 0))],
        out_specs=pl.BlockSpec((rows, 2 * ff), lambda i: (i, 0)),
        out_shape=jax.ShapeDtypeStruct((tokens, 2 * ff), jnp.bfloat16),
        cost_estimate=pl.CostEstimate(flops=16_000_000_000, bytes_accessed=50_000_000, transcendentals=3_200_000),
        name='mlp_bwd',
    )(gu, grad_act)


def pack_in_kernel(kv_heads, q_ref, k_ref, v_ref, gate_ref, up_ref, out_ref):
    q_w, k_w = q_ref.shape[1] // kv_heads, k_ref.shape[1] // kv_heads
    for g in range(kv_heads):
        lo = g * (q_w + 2 * k_w)
        out_ref[:, lo:lo + q_w] = q_ref[:, g * q_w:(g + 1) * q_w]
        out_ref[:, lo + q_w:lo + q_w + k_w] = k_ref[:, g * k_w:(g + 1) * k_w]
        out_ref[:, lo + q_w + k_w:lo + q_w + 2 * k_w] = v_ref[:, g * k_w:(g + 1) * k_w]
    lo = kv_heads * (q_w + 2 * k_w)
    out_ref[:, lo:lo + gate_ref.shape[1]] = gate_ref[...]
    out_ref[:, lo + gate_ref.shape[1]:] = up_ref[...]


def pack_in(kv_heads, *shards):
    width = sum(w.shape[1] for w in shards)
    return pl.pallas_call(
        functools.partial(pack_in_kernel, kv_heads),
        out_shape=jax.ShapeDtypeStruct((shards[0].shape[0], width), shards[0].dtype),
        cost_estimate=pl.CostEstimate(flops=1_000_000, bytes_accessed=2_600_000, transcendentals=0),
        name='pack_in',
    )(*shards)


def pack_tail_kernel(kv_heads, n_rep, hd, qkv_ref, out_rows_ref, out_ref):
    rows, dim = qkv_ref.shape[0], out_ref.shape[1]
    group, n_q = (n_rep + 2) * hd, kv_heads * n_rep * hd // dim
    per = kv_heads // n_q
    for g in range(kv_heads):
        lo, p = g * group, (g // per) * rows
        out_ref[p:p + rows, (g % per) * n_rep * hd:(g % per + 1) * n_rep * hd] = qkv_ref[:, lo:lo + n_rep * hd]
        for j in range(2):
            p = (n_q + j) * rows
            out_ref[p:p + rows, g * hd:(g + 1) * hd] = qkv_ref[:, lo + (n_rep + j) * hd:lo + (n_rep + j + 1) * hd]
    out_ref[(n_q + 2) * rows:] = out_rows_ref[...]


def pack_tail(part_qkv, part_out, n_chip, kv_heads, n_rep, hd):
    rows, out_rows, dim = part_qkv.shape[0] // n_chip, part_out.shape[0] // n_chip, part_out.shape[1]
    block = part_qkv.shape[1] // dim * rows + out_rows
    return pl.pallas_call(
        functools.partial(pack_tail_kernel, kv_heads, n_rep, hd),
        grid=(n_chip,),
        in_specs=[pl.BlockSpec((rows, part_qkv.shape[1]), lambda i: (i, 0)), pl.BlockSpec((out_rows, dim), lambda i: (i, 0))],
        out_specs=pl.BlockSpec((block, dim), lambda i: (i, 0)),
        out_shape=jax.ShapeDtypeStruct((n_chip * block, dim), jnp.float32),
        cost_estimate=pl.CostEstimate(flops=8_000_000_000, bytes_accessed=25_000_000, transcendentals=0),
        name='pack_tail',
    )(part_qkv, part_out)


def solution(mesh):
    n_dev = mesh.shape[AXIS_NAME]
    n_chip = n_dev // 2
    pairs = [(i, i ^ 1) for i in range(n_dev)]
    same_core = [[2 * k + core for k in range(n_chip)] for core in range(2)]
    row_spec = P(AXIS_NAME, None)
    vec_spec = P(AXIS_NAME)
    full_spec = P(None)
    batch_spec = P(AXIS_NAME, None, None)
    weight_specs = (vec_spec, row_spec, row_spec, row_spec, full_spec, full_spec, row_spec, vec_spec, row_spec, row_spec, row_spec)

    def gather(shard):
        return lax.all_gather(shard, AXIS_NAME, tiled=True)

    def scatter_chips(part):
        return lax.psum_scatter(part, AXIS_NAME, scatter_dimension=0, tiled=True, axis_index_groups=same_core)

    def swap_core(part):
        return lax.ppermute(part, AXIS_NAME, pairs)

    def device_step(tokens, positions, table_shard, attn_norm, w_query, w_key, w_value, q_norm, k_norm, w_out, mlp_norm, w_gate, w_up, w_down, dy_out):
        me = lax.axis_index(AXIS_NAME)
        core = lax.rem(me, 2)
        batch, seq = tokens.shape
        rows_local, dim = table_shard.shape
        n_tok = batch * seq
        hd = q_norm.shape[0]
        kv_heads = w_key.shape[1] // hd
        n_rep = w_query.shape[1] // w_key.shape[1]
        ff = w_gate.shape[1]
        shard_rows = w_query.shape[0]

        def near_far(blocks, axis):
            return lax.dynamic_index_in_dim(blocks, core, axis, False), lax.dynamic_index_in_dim(blocks, 1 - core, axis, False)

        small = jnp.concatenate([tokens.reshape(-1).astype(jnp.float32), attn_norm.astype(jnp.float32), mlp_norm.astype(jnp.float32)])
        small = lax.all_gather(small, AXIS_NAME)
        attn_gain = small[:, n_tok:n_tok + shard_rows].reshape(1, dim)
        mlp_gain = small[:, n_tok + shard_rows:].reshape(1, dim)

        in_shard = pack_in(kv_heads, w_query, w_key, w_value, w_gate, w_up)
        w_in = gather(in_shard)
        qkv_cols = w_query.shape[1] + 2 * w_key.shape[1]
        wqkv = w_in[:, :qkv_cols]
        wgu = w_in[:, qkv_cols:]
        wqkv, wgu = lax.optimization_barrier((wqkv, wgu))
        small, _ = lax.optimization_barrier((small, in_shard))
        all_ids = small[:, :n_tok].astype(jnp.int32).reshape(n_chip, 2, batch, seq)

        def local_rows(ids, owner):
            local = ids - owner * rows_local
            return local, ((local >= 0) & (local < rows_local))[:, None]

        def pick(ids):
            local, _ = local_rows(ids, me)
            return jnp.take(table_shard, jnp.clip(local, 0, rows_local - 1), axis=0, mode='clip')

        seq_pad = -(-seq // 48) * 48

        def lookup(b):
            ids = jnp.pad(all_ids[:, :, b], ((0, 0), (0, 0), (0, seq_pad - seq)), constant_values=-1)
            near, far = near_far(ids, 1)
            near, far = near.reshape(-1), far.reshape(-1)
            near_rows, far_rows = pick(near), pick(far)
            recv = swap_core(far_rows)
            zero = jnp.zeros((), table_shard.dtype)
            merged = jnp.where(local_rows(near, me)[1], near_rows, jnp.where(local_rows(near, me + 1 - 2 * core)[1], recv, zero))
            return merged

        merged = []
        for b in range(batch):
            merged.append(lookup(b))
            merged[b], all_ids = lax.optimization_barrier((merged[b], all_ids))
        merged[-1], w_out, w_down = lax.optimization_barrier((merged[-1], w_out, w_down))
        x_emb = [scatter_chips(m)[:seq] for m in merged]
        wo = gather(w_out)
        wdown = gather(w_down)

        cos_t, sin_t = rope_tables(positions, hd)
        q_gain = q_norm.astype(jnp.float32)[None]
        k_gain = k_norm.astype(jnp.float32)[None]

        normed1, norm1_inv, attn_in, qkv, heads = [], [], [], [], ()
        for b in range(batch):
            if b:
                x_emb[b], heads = lax.optimization_barrier((x_emb[b], heads))
            normed_b, inv_b = norm_fwd(x_emb[b])
            normed1.append(normed_b)
            norm1_inv.append(inv_b)
            attn_in.append((normed_b * attn_gain).astype(jnp.bfloat16))
            qkv.append(dot_nn(attn_in[b], wqkv).astype(jnp.bfloat16))
            heads = attn_fwd(b, heads, qkv[b], cos_t, sin_t, q_gain, k_gain, batch, kv_heads, n_rep, hd)
        heads, *heads_rep = heads
        x_all = jnp.concatenate(x_emb, axis=0)
        hidden = (x_all.astype(jnp.float32) + dot_nn(heads, wo)).astype(jnp.bfloat16)
        normed2, norm2_inv = norm_fwd(hidden)
        mlp_in = (normed2 * mlp_gain).astype(jnp.bfloat16)
        gu = dot_nn(mlp_in, wgu)

        act, near_act, far_act = mlp_act(gu, core, n_chip)

        dy = dy_out.reshape(n_tok, dim)
        part_down = kdot_nn(near_act, dy) + swap_core(kdot_nn(far_act, dy))
        dy_b, part_down = lax.optimization_barrier((dy, part_down))
        g_down = scatter_chips(part_down)
        grad_act = dot_nt(dy_b, wdown)
        dgu = mlp_bwd(gu, grad_act)

        row_ids = jnp.arange(dim)

        def split_cores(a, block):
            pad = jnp.full((n_chip, 2, block - shard_rows), -1, row_ids.dtype)
            order = jnp.concatenate([row_ids.reshape(n_chip, 2, shard_rows), pad], axis=2)
            order = jnp.concatenate([part.reshape(-1) for part in near_far(order, 1)])
            select = (row_ids[:, None] == order[None, :]).astype(jnp.bfloat16)
            both = dot_nn(a, select).astype(jnp.bfloat16)
            return both[:, :n_chip * block], both[:, n_chip * block:]

        near2, far2 = split_cores(mlp_in, shard_rows)
        far_gu, dgu = lax.optimization_barrier((dot_tn(far2, dgu), dgu))
        recv_gu = swap_core(far_gu)
        grad_mlp_in = dot_nt(dgu, wgu)
        part_gu = dot_tn(near2, dgu) + recv_gu
        grad_mlp_norm = jnp.sum(grad_mlp_in * normed2, axis=0)
        grad_hidden = dy.astype(jnp.float32) + norm_bwd(grad_mlp_in, normed2, norm2_inv, mlp_gain)
        hidden_b = grad_hidden.astype(jnp.bfloat16)
        hidden_b, part_gu = lax.optimization_barrier((hidden_b, part_gu))
        g_gu = scatter_chips(part_gu)

        near_h = jnp.where(core == 0, heads_rep[0], heads_rep[1])
        far_h = jnp.where(core == 0, heads_rep[1], heads_rep[0])
        recv_out = swap_core(dot_tn(far_h, hidden_b))
        grad_heads = dot_nt(hidden_b, wo).astype(jnp.bfloat16)
        part_out = dot_tn(near_h, hidden_b) + recv_out
        local_ids = (all_ids - me * rows_local).reshape(n_dev, batch, seq)
        slots = jnp.where((local_ids >= 0) & (local_ids < rows_local), local_ids, rows_local)
        grad_attn_norm, grad_q_norm, grad_k_norm = 0.0, 0.0, 0.0
        dqkv, all_rows = (), []
        for b in range(batch):
            rows = slice(b * seq, (b + 1) * seq)
            dqkv, dqg, dkg = attn_bwd(b, dqkv, qkv[b], grad_heads, cos_t, sin_t, q_gain, k_gain, batch, kv_heads, n_rep, hd)
            grad_attn_in = dot_nt(dqkv[rows], wqkv)
            grad_attn_norm += jnp.sum(grad_attn_in * normed1[b], axis=0)
            grad_q_norm += jnp.sum(dqg, axis=0)
            grad_k_norm += jnp.sum(dkg, axis=0)
            grad_x = grad_hidden[rows] + norm_bwd(grad_attn_in, normed1[b], norm1_inv[b], attn_gain)
            grad_x, dqkv = lax.optimization_barrier((row_major(grad_x), dqkv))
            all_rows.append(gather(grad_x))
            dqkv = (dqkv,)
        dqkv, = dqkv
        near1, far1 = split_cores(jnp.concatenate(attn_in, axis=0), shard_rows)
        far_qkv = dot_tn(far1, dqkv)
        part_qkv = dot_tn(near1, dqkv) + swap_core(far_qkv)
        part_tail = pack_tail(part_qkv, part_out, n_chip, kv_heads, n_rep, hd)
        g_tail = scatter_chips(part_tail)
        layer_out = (hidden.astype(jnp.float32) + dot_nn(act, wdown)).astype(jnp.bfloat16)

        vec = jnp.concatenate([grad_attn_norm, grad_mlp_norm, grad_q_norm, grad_k_norm])
        vec, layer_out, _ = lax.optimization_barrier((vec, layer_out, part_tail))
        vec = jnp.sum(lax.all_gather(vec, AXIS_NAME), axis=0)
        g_attn_norm = lax.dynamic_slice_in_dim(vec[:dim], me * shard_rows, shard_rows)
        g_mlp_norm = lax.dynamic_slice_in_dim(vec[dim:2 * dim], me * shard_rows, shard_rows)
        g_q_norm = vec[2 * dim:2 * dim + hd]
        g_k_norm = vec[2 * dim + hd:]

        d_table = jnp.zeros((rows_local, dim), jnp.float32)
        for b in range(batch):
            d_table = d_table.at[slots[:, b].reshape(-1)].add(all_rows[b], mode='drop')

        n_q = w_query.shape[1] // dim
        g_query = jnp.concatenate([g_tail[p * shard_rows:(p + 1) * shard_rows] for p in range(n_q)], axis=1)
        g_key = g_tail[n_q * shard_rows:(n_q + 1) * shard_rows]
        g_value = g_tail[(n_q + 1) * shard_rows:(n_q + 2) * shard_rows]
        g_out = g_tail[(n_q + 2) * shard_rows:]
        return (layer_out.reshape(dy_out.shape), d_table, g_attn_norm, g_query, g_key, g_value, g_q_norm, g_k_norm, g_out, g_mlp_norm, g_gu[:, :ff], g_gu[:, ff:], g_down)

    return jax.shard_map(device_step, mesh=mesh, in_specs=(row_spec, row_spec, row_spec) + weight_specs + (batch_spec,), out_specs=(batch_spec, row_spec) + weight_specs, check_vma=False)
```

```python
import functools
import math
import jax
import jax.numpy as jnp
from jax import lax
from jax.experimental import pallas as pl
from jax.experimental.layout import Layout, with_layout_constraint
from jax.experimental.pallas import tpu as pltpu
from jax.sharding import PartitionSpec as P

NORM_EPS = 1e-6
ROPE_THETA = 1.0e6
AXIS_NAME = 'fsdp'
NEG = -1e30


def split_rows(a):
    return a.reshape(2, a.shape[0] // 2, a.shape[1])


def kdot_nn(a, b):
    return lax.dot_general(a, b, (((1,), (0,)), ((), ())), preferred_element_type=jnp.float32)


def kdot_nt(a, b):
    return lax.dot_general(a, b, (((1,), (1,)), ((), ())), preferred_element_type=jnp.float32)


def dot_nn(a, b):
    return lax.dot_general(split_rows(a), b, (((2,), (0,)), ((), ())), preferred_element_type=jnp.float32).reshape(a.shape[0], -1)


def dot_nt(a, b):
    return lax.dot_general(split_rows(a), b, (((2,), (1,)), ((), ())), preferred_element_type=jnp.float32).reshape(a.shape[0], -1)


def dot_tn(a, b):
    return lax.dot_general(split_rows(a), split_rows(b), (((0, 1), (0, 1)), ((), ())), preferred_element_type=jnp.float32)


def row_major(a):
    return with_layout_constraint(a, Layout(major_to_minor=tuple(range(a.ndim))))


def norm_fwd(values):
    values_f = values.astype(jnp.float32)
    inv_rms = lax.rsqrt(jnp.mean(values_f * values_f, axis=-1, keepdims=True) + NORM_EPS)
    return values_f * inv_rms, inv_rms


def norm_bwd(grad_out, normed, inv_rms, gain_f):
    grad_normed = grad_out * gain_f
    mean_term = jnp.mean(grad_normed * normed, axis=-1, keepdims=True)
    return inv_rms * (grad_normed - normed * mean_term)


def rope_tables(positions, head_dim):
    half_dim = head_dim // 2
    inv_freq = jnp.exp(jnp.arange(half_dim, dtype=jnp.float32) * (-2.0 * math.log(ROPE_THETA) / head_dim))
    angles = positions.astype(jnp.float32).reshape(-1, 1) * inv_freq
    cos_t, sin_t = jnp.cos(angles), jnp.sin(angles)
    return jnp.concatenate([cos_t, cos_t], axis=-1), jnp.concatenate([-sin_t, sin_t], axis=-1)


def rope(values, cos_t, sin_t):
    return values * cos_t + pltpu.roll(values, values.shape[-1] // 2, 1) * sin_t


def attn_fwd_kernel(n_rep, hd, chunk, n_alias, qkv_ref, cos_ref, sin_ref, qg_ref, kg_ref, *rest):
    out_ref, *rep_refs = rest[n_alias:]
    seq = qkv_ref.shape[0]
    scale = hd ** -0.5
    cos_t, sin_t = cos_ref[...], sin_ref[...]
    k_n, _ = norm_fwd(qkv_ref[:, n_rep * hd:(n_rep + 1) * hd])
    k_rot = rope(k_n * kg_ref[...], cos_t, sin_t).astype(jnp.bfloat16)
    v_t = qkv_ref[:, (n_rep + 1) * hd:(n_rep + 2) * hd].astype(jnp.float32).T.astype(jnp.bfloat16)
    for rep in range(n_rep):
        q_n, _ = norm_fwd(qkv_ref[:, rep * hd:(rep + 1) * hd])
        q_rot = rope(q_n * qg_ref[...], cos_t, sin_t).astype(jnp.bfloat16)
        for lo in range(0, seq, chunk):
            end = lo + chunk
            s = kdot_nt(k_rot[:end], q_rot[lo:end]) * scale
            keys = lax.broadcasted_iota(jnp.int32, s.shape, 0)
            qpos = lax.broadcasted_iota(jnp.int32, s.shape, 1) + lo
            s = jnp.where(qpos >= keys, s, NEG)
            e = jnp.exp(s - jnp.max(s, axis=0, keepdims=True))
            p = e * (1.0 / jnp.sum(e, axis=0, keepdims=True))
            o = kdot_nn(v_t[:, :end], p.astype(jnp.bfloat16)).T
            out_ref[lo:end, rep * hd:(rep + 1) * hd] = o.astype(jnp.bfloat16)
            rep_refs[rep][lo:end] = o.astype(jnp.bfloat16)


def attn_fwd(b, prev, qkv, cos_t, sin_t, q_gain, k_gain, batch, kv_heads, n_rep, hd):
    seq, width = qkv.shape
    gw = width // kv_heads
    return pl.pallas_call(
        functools.partial(attn_fwd_kernel, n_rep, hd, seq // 2, len(prev)),
        grid=(kv_heads,),
        in_specs=[pl.BlockSpec((seq, gw), lambda g: (0, g)),
                  pl.BlockSpec((seq, hd), lambda g: (b, 0)),
                  pl.BlockSpec((seq, hd), lambda g: (b, 0)),
                  pl.BlockSpec((1, hd), lambda g: (0, 0)),
                  pl.BlockSpec((1, hd), lambda g: (0, 0))] + [pl.BlockSpec(memory_space=pl.ANY)] * len(prev),
        out_specs=[pl.BlockSpec((seq, n_rep * hd), lambda g: (b, g))] + [pl.BlockSpec((seq, hd), lambda g: (b, g))] * n_rep,
        out_shape=[jax.ShapeDtypeStruct((seq * batch, kv_heads * n_rep * hd), jnp.bfloat16)] + [jax.ShapeDtypeStruct((seq * batch, kv_heads * hd), jnp.bfloat16)] * n_rep,
        input_output_aliases={5 + n: n for n in range(len(prev))},
        cost_estimate=pl.CostEstimate(flops=12_000_000_000, bytes_accessed=8_000_000, transcendentals=4_200_000),
        name='attn_fwd',
    )(qkv, cos_t, sin_t, q_gain, k_gain, *prev)


def attn_bwd_kernel(n_rep, hd, chunk, n_alias, qkv_ref, do_ref, cos_ref, sin_ref, qg_ref, kg_ref, *rest):
    dqkv_ref, dqg_ref, dkg_ref, dk_acc, dv_acc = rest[n_alias:]
    seq = qkv_ref.shape[0]
    scale = hd ** -0.5
    cos_t, sin_t = cos_ref[...], sin_ref[...]
    qg, kg = qg_ref[...], kg_ref[...]

    @pl.when(pl.program_id(0) == 0)
    def _():
        dqg_ref[...] = jnp.zeros_like(dqg_ref)
        dkg_ref[...] = jnp.zeros_like(dkg_ref)

    k_n, k_inv = norm_fwd(qkv_ref[:, n_rep * hd:(n_rep + 1) * hd])
    k_rot_f = rope(k_n * kg, cos_t, sin_t)
    k_rot = k_rot_f.astype(jnp.bfloat16)
    k_rot_t = k_rot_f.T.astype(jnp.bfloat16)
    v_raw = qkv_ref[:, (n_rep + 1) * hd:(n_rep + 2) * hd]
    dk_acc[...] = jnp.zeros_like(dk_acc)
    dv_acc[...] = jnp.zeros_like(dv_acc)
    for rep in range(n_rep):
        q_n, q_inv = norm_fwd(qkv_ref[:, rep * hd:(rep + 1) * hd])
        q_rot = rope(q_n * qg, cos_t, sin_t).astype(jnp.bfloat16)
        dq_parts = []
        for lo in range(0, seq, chunk):
            end = lo + chunk
            q_c = q_rot[lo:end]
            do_c = do_ref[lo:end, rep * hd:(rep + 1) * hd]
            s = kdot_nt(k_rot[:end], q_c) * scale
            keys = lax.broadcasted_iota(jnp.int32, s.shape, 0)
            qpos = lax.broadcasted_iota(jnp.int32, s.shape, 1) + lo
            s = jnp.where(qpos >= keys, s, NEG)
            e = jnp.exp(s - jnp.max(s, axis=0, keepdims=True))
            p = e * (1.0 / jnp.sum(e, axis=0, keepdims=True))
            dv_acc[:end] += kdot_nn(p.astype(jnp.bfloat16), do_c)
            dp = kdot_nt(v_raw[:end], do_c)
            delta = jnp.sum(dp * p, axis=0, keepdims=True)
            ds = (p * (dp - delta) * scale).astype(jnp.bfloat16)
            dk_acc[:end] += kdot_nn(ds, q_c)
            dq_parts.append(kdot_nn(k_rot_t[:, :end], ds).T)
        dq = jnp.concatenate(dq_parts, axis=0)
        dqt = dq * cos_t - pltpu.roll(dq, hd // 2, 1) * sin_t
        dqg_ref[...] += jnp.sum((dqt * q_n).reshape(seq // 8, 8, hd), axis=0)
        dqkv_ref[:, rep * hd:(rep + 1) * hd] = norm_bwd(dqt, q_n, q_inv, qg).astype(jnp.bfloat16)
    dk = dk_acc[...]
    dkt = dk * cos_t - pltpu.roll(dk, hd // 2, 1) * sin_t
    dkg_ref[...] += jnp.sum((dkt * k_n).reshape(seq // 8, 8, hd), axis=0)
    dqkv_ref[:, n_rep * hd:(n_rep + 1) * hd] = norm_bwd(dkt, k_n, k_inv, kg).astype(jnp.bfloat16)
    dqkv_ref[:, (n_rep + 1) * hd:(n_rep + 2) * hd] = dv_acc[...].astype(jnp.bfloat16)


def attn_bwd(b, prev, qkv, do, cos_t, sin_t, q_gain, k_gain, batch, kv_heads, n_rep, hd):
    seq, width = qkv.shape
    tokens = seq * batch
    gw = width // kv_heads
    return pl.pallas_call(
        functools.partial(attn_bwd_kernel, n_rep, hd, seq // 2, len(prev)),
        grid=(kv_heads,),
        in_specs=[pl.BlockSpec((seq, gw), lambda g: (0, g)),
                  pl.BlockSpec((seq, n_rep * hd), lambda g: (b, g)),
                  pl.BlockSpec((seq, hd), lambda g: (b, 0)),
                  pl.BlockSpec((seq, hd), lambda g: (b, 0)),
                  pl.BlockSpec((1, hd), lambda g: (0, 0)),
                  pl.BlockSpec((1, hd), lambda g: (0, 0))] + [pl.BlockSpec(memory_space=pl.ANY)] * len(prev),
        out_specs=[pl.BlockSpec((seq, gw), lambda g: (b, g)),
                   pl.BlockSpec((8, hd), lambda g: (0, 0)),
                   pl.BlockSpec((8, hd), lambda g: (0, 0))],
        out_shape=[jax.ShapeDtypeStruct((tokens, width), jnp.bfloat16),
                   jax.ShapeDtypeStruct((8, hd), jnp.float32),
                   jax.ShapeDtypeStruct((8, hd), jnp.float32)],
        input_output_aliases={6: 0} if prev else {},
        scratch_shapes=[pltpu.VMEM((seq, hd), jnp.float32), pltpu.VMEM((seq, hd), jnp.float32)],
        cost_estimate=pl.CostEstimate(flops=25_000_000_000, bytes_accessed=14_000_000, transcendentals=4_200_000),
        name='attn_bwd',
    )(qkv, do, cos_t, sin_t, q_gain, k_gain, *prev)


def mlp_fwd_kernel(core_ref, x_ref, w_ref, gu_ref, act_ref, near_ref, far_ref):
    tile, block, chunk = act_ref.shape[1], near_ref.shape[0], 256
    first = core_ref[0] == 0
    for lo in range(0, x_ref.shape[0], chunk):
        gu = kdot_nn(x_ref[lo:lo + chunk], w_ref[...])
        gu_ref[lo:lo + chunk] = gu
        gate = gu[:, :tile]
        act = gate * jax.nn.sigmoid(gate) * gu[:, tile:]
        act_ref[lo:lo + chunk] = act.astype(jnp.bfloat16)
        act_t = act.T.astype(jnp.bfloat16)
        near_ref[:, lo:lo + chunk] = jnp.where(first, act_t[:block], act_t[block:])
        far_ref[:, lo:lo + chunk] = jnp.where(first, act_t[block:], act_t[:block])


def mlp_fwd(x, wgu, core, n_chip):
    tokens, dim = x.shape
    ff = wgu.shape[1] // 2
    tile = ff // n_chip
    half = pl.BlockSpec((tile // 2, tokens), lambda i: (i, 0))
    return pl.pallas_call(
        mlp_fwd_kernel,
        grid=(n_chip,),
        in_specs=[pl.BlockSpec(memory_space=pltpu.SMEM), pl.BlockSpec((tokens, dim), lambda i: (0, 0)), pl.BlockSpec((dim, 2 * tile), lambda i: (0, i))],
        out_specs=[pl.BlockSpec((tokens, 2 * tile), lambda i: (0, i)), pl.BlockSpec((tokens, tile), lambda i: (0, i)), half, half],
        out_shape=[jax.ShapeDtypeStruct((tokens, 2 * ff), jnp.float32), jax.ShapeDtypeStruct((tokens, ff), jnp.bfloat16),
                   jax.ShapeDtypeStruct((ff // 2, tokens), jnp.bfloat16), jax.ShapeDtypeStruct((ff // 2, tokens), jnp.bfloat16)],
        cost_estimate=pl.CostEstimate(flops=16_000_000_000, bytes_accessed=52_000_000, transcendentals=3_200_000),
        name='mlp_fwd',
    )(core.reshape(1), x, wgu)


def mlp_bwd_kernel(dy_ref, w_ref, gu_ref, out_ref):
    tile, chunk = w_ref.shape[0], 256
    for lo in range(0, dy_ref.shape[0], chunk):
        grad_act = kdot_nt(dy_ref[lo:lo + chunk], w_ref[...])
        gate, up = gu_ref[lo:lo + chunk, :tile], gu_ref[lo:lo + chunk, tile:]
        sig = jax.nn.sigmoid(gate)
        out_ref[lo:lo + chunk, :tile] = (grad_act * up * sig * (1.0 + gate * (1.0 - sig))).astype(jnp.bfloat16)
        out_ref[lo:lo + chunk, tile:] = (grad_act * gate * sig).astype(jnp.bfloat16)


def mlp_bwd(dy, wdown, gu, n_chip):
    tokens, dim = dy.shape
    tile = wdown.shape[0] // n_chip
    return pl.pallas_call(
        mlp_bwd_kernel,
        grid=(n_chip,),
        in_specs=[pl.BlockSpec((tokens, dim), lambda i: (0, 0)), pl.BlockSpec((tile, dim), lambda i: (i, 0)), pl.BlockSpec((tokens, 2 * tile), lambda i: (0, i))],
        out_specs=pl.BlockSpec((tokens, 2 * tile), lambda i: (0, i)),
        out_shape=jax.ShapeDtypeStruct(gu.shape, jnp.bfloat16),
        cost_estimate=pl.CostEstimate(flops=12_000_000_000, bytes_accessed=46_000_000, transcendentals=3_200_000),
        name='mlp_bwd',
    )(dy, wdown, gu)


def unpack_gu_kernel(n_tiles, in_ref, gate_ref, up_ref):
    tile = gate_ref.shape[1] // n_tiles
    for i in range(n_tiles):
        gate_ref[:, i * tile:(i + 1) * tile] = in_ref[:, 2 * i * tile:(2 * i + 1) * tile]
        up_ref[:, i * tile:(i + 1) * tile] = in_ref[:, (2 * i + 1) * tile:(2 * i + 2) * tile]


def unpack_gu(g_gu, n_tiles):
    shape = jax.ShapeDtypeStruct((g_gu.shape[0], g_gu.shape[1] // 2), g_gu.dtype)
    return pl.pallas_call(functools.partial(unpack_gu_kernel, n_tiles), out_shape=[shape, shape], name='unpack_gu')(g_gu)


def pack_in_kernel(kv_heads, n_tiles, q_ref, k_ref, v_ref, gate_ref, up_ref, out_ref):
    q_w, k_w = q_ref.shape[1] // kv_heads, k_ref.shape[1] // kv_heads
    for g in range(kv_heads):
        lo = g * (q_w + 2 * k_w)
        out_ref[:, lo:lo + q_w] = q_ref[:, g * q_w:(g + 1) * q_w]
        out_ref[:, lo + q_w:lo + q_w + k_w] = k_ref[:, g * k_w:(g + 1) * k_w]
        out_ref[:, lo + q_w + k_w:lo + q_w + 2 * k_w] = v_ref[:, g * k_w:(g + 1) * k_w]
    lo = kv_heads * (q_w + 2 * k_w)
    tile = gate_ref.shape[1] // n_tiles
    for i in range(n_tiles):
        out_ref[:, lo + 2 * i * tile:lo + (2 * i + 1) * tile] = gate_ref[:, i * tile:(i + 1) * tile]
        out_ref[:, lo + (2 * i + 1) * tile:lo + (2 * i + 2) * tile] = up_ref[:, i * tile:(i + 1) * tile]


def pack_in(kv_heads, n_tiles, *shards):
    width = sum(w.shape[1] for w in shards)
    return pl.pallas_call(
        functools.partial(pack_in_kernel, kv_heads, n_tiles),
        out_shape=jax.ShapeDtypeStruct((shards[0].shape[0], width), shards[0].dtype),
        cost_estimate=pl.CostEstimate(flops=1_000_000, bytes_accessed=2_600_000, transcendentals=0),
        name='pack_in',
    )(*shards)


def pack_tail_kernel(kv_heads, n_rep, hd, qkv_ref, out_rows_ref, out_ref):
    rows, dim = qkv_ref.shape[0], out_ref.shape[1]
    group, n_q = (n_rep + 2) * hd, kv_heads * n_rep * hd // dim
    per = kv_heads // n_q
    for g in range(kv_heads):
        lo, p = g * group, (g // per) * rows
        out_ref[p:p + rows, (g % per) * n_rep * hd:(g % per + 1) * n_rep * hd] = qkv_ref[:, lo:lo + n_rep * hd]
        for j in range(2):
            p = (n_q + j) * rows
            out_ref[p:p + rows, g * hd:(g + 1) * hd] = qkv_ref[:, lo + (n_rep + j) * hd:lo + (n_rep + j + 1) * hd]
    out_ref[(n_q + 2) * rows:] = out_rows_ref[...]


def pack_tail(part_qkv, part_out, n_chip, kv_heads, n_rep, hd):
    rows, out_rows, dim = part_qkv.shape[0] // n_chip, part_out.shape[0] // n_chip, part_out.shape[1]
    block = part_qkv.shape[1] // dim * rows + out_rows
    return pl.pallas_call(
        functools.partial(pack_tail_kernel, kv_heads, n_rep, hd),
        grid=(n_chip,),
        in_specs=[pl.BlockSpec((rows, part_qkv.shape[1]), lambda i: (i, 0)), pl.BlockSpec((out_rows, dim), lambda i: (i, 0))],
        out_specs=pl.BlockSpec((block, dim), lambda i: (i, 0)),
        out_shape=jax.ShapeDtypeStruct((n_chip * block, dim), jnp.float32),
        cost_estimate=pl.CostEstimate(flops=8_000_000_000, bytes_accessed=25_000_000, transcendentals=0),
        name='pack_tail',
    )(part_qkv, part_out)


def solution(mesh):
    n_dev = mesh.shape[AXIS_NAME]
    n_chip = n_dev // 2
    pairs = [(i, i ^ 1) for i in range(n_dev)]
    same_core = [[2 * k + core for k in range(n_chip)] for core in range(2)]
    row_spec = P(AXIS_NAME, None)
    vec_spec = P(AXIS_NAME)
    full_spec = P(None)
    batch_spec = P(AXIS_NAME, None, None)
    weight_specs = (vec_spec, row_spec, row_spec, row_spec, full_spec, full_spec, row_spec, vec_spec, row_spec, row_spec, row_spec)

    def gather(shard):
        return lax.all_gather(shard, AXIS_NAME, tiled=True)

    def scatter_chips(part):
        return lax.psum_scatter(part, AXIS_NAME, scatter_dimension=0, tiled=True, axis_index_groups=same_core)

    def swap_core(part):
        return lax.ppermute(part, AXIS_NAME, pairs)

    def device_step(tokens, positions, table_shard, attn_norm, w_query, w_key, w_value, q_norm, k_norm, w_out, mlp_norm, w_gate, w_up, w_down, dy_out):
        me = lax.axis_index(AXIS_NAME)
        core = lax.rem(me, 2)
        batch, seq = tokens.shape
        rows_local, dim = table_shard.shape
        n_tok = batch * seq
        hd = q_norm.shape[0]
        kv_heads = w_key.shape[1] // hd
        n_rep = w_query.shape[1] // w_key.shape[1]
        shard_rows = w_query.shape[0]

        def near_far(blocks, axis):
            return lax.dynamic_index_in_dim(blocks, core, axis, False), lax.dynamic_index_in_dim(blocks, 1 - core, axis, False)

        small = jnp.concatenate([tokens.reshape(-1).astype(jnp.float32), attn_norm.astype(jnp.float32), mlp_norm.astype(jnp.float32)])
        small = lax.all_gather(small, AXIS_NAME)
        attn_gain = small[:, n_tok:n_tok + shard_rows].reshape(1, dim)
        mlp_gain = small[:, n_tok + shard_rows:].reshape(1, dim)

        in_shard = pack_in(kv_heads, n_chip, w_query, w_key, w_value, w_gate, w_up)
        w_in = gather(in_shard)
        qkv_cols = w_query.shape[1] + 2 * w_key.shape[1]
        wqkv = w_in[:, :qkv_cols]
        wgu = w_in[:, qkv_cols:]
        wqkv, wgu = lax.optimization_barrier((wqkv, wgu))
        small, _ = lax.optimization_barrier((small, in_shard))
        all_ids = small[:, :n_tok].astype(jnp.int32).reshape(n_chip, 2, batch, seq)

        def local_rows(ids, owner):
            local = ids - owner * rows_local
            return local, ((local >= 0) & (local < rows_local))[:, None]

        def pick(ids):
            local, _ = local_rows(ids, me)
            return jnp.take(table_shard, jnp.clip(local, 0, rows_local - 1), axis=0, mode='clip')

        seq_pad = -(-seq // 48) * 48

        def lookup(b):
            ids = jnp.pad(all_ids[:, :, b], ((0, 0), (0, 0), (0, seq_pad - seq)), constant_values=-1)
            near, far = near_far(ids, 1)
            near, far = near.reshape(-1), far.reshape(-1)
            near_rows, far_rows = pick(near), pick(far)
            recv = swap_core(far_rows)
            zero = jnp.zeros((), table_shard.dtype)
            merged = jnp.where(local_rows(near, me)[1], near_rows, jnp.where(local_rows(near, me + 1 - 2 * core)[1], recv, zero))
            return merged

        merged = []
        for b in range(batch):
            merged.append(lookup(b))
            merged[b], all_ids = lax.optimization_barrier((merged[b], all_ids))
        merged[-1], w_out, w_down = lax.optimization_barrier((merged[-1], w_out, w_down))
        x_emb = [scatter_chips(m)[:seq] for m in merged]
        wo = gather(w_out)
        wdown = gather(w_down)

        cos_t, sin_t = rope_tables(positions, hd)
        q_gain = q_norm.astype(jnp.float32)[None]
        k_gain = k_norm.astype(jnp.float32)[None]

        normed1, norm1_inv, attn_in, qkv, heads = [], [], [], [], ()
        for b in range(batch):
            if b:
                x_emb[b], heads = lax.optimization_barrier((x_emb[b], heads))
            normed_b, inv_b = norm_fwd(x_emb[b])
            normed1.append(normed_b)
            norm1_inv.append(inv_b)
            attn_in.append((normed_b * attn_gain).astype(jnp.bfloat16))
            qkv.append(dot_nn(attn_in[b], wqkv).astype(jnp.bfloat16))
            heads = attn_fwd(b, heads, qkv[b], cos_t, sin_t, q_gain, k_gain, batch, kv_heads, n_rep, hd)
        heads, *heads_rep = heads
        x_all = jnp.concatenate(x_emb, axis=0)
        hidden = (x_all.astype(jnp.float32) + dot_nn(heads, wo)).astype(jnp.bfloat16)
        normed2, norm2_inv = norm_fwd(hidden)
        mlp_in = (normed2 * mlp_gain).astype(jnp.bfloat16)
        gu, act, near_act, far_act = mlp_fwd(mlp_in, wgu, core, n_chip)


        dy = dy_out.reshape(n_tok, dim)
        part_down = kdot_nn(near_act, dy) + swap_core(kdot_nn(far_act, dy))
        dy_b, part_down = lax.optimization_barrier((dy, part_down))
        g_down = scatter_chips(part_down)
        dgu = mlp_bwd(dy_b, wdown, gu, n_chip)

        row_ids = jnp.arange(dim)

        def split_cores(a, block):
            pad = jnp.full((n_chip, 2, block - shard_rows), -1, row_ids.dtype)
            order = jnp.concatenate([row_ids.reshape(n_chip, 2, shard_rows), pad], axis=2)
            order = jnp.concatenate([part.reshape(-1) for part in near_far(order, 1)])
            select = (row_ids[:, None] == order[None, :]).astype(jnp.bfloat16)
            both = dot_nn(a, select).astype(jnp.bfloat16)
            return both[:, :n_chip * block], both[:, n_chip * block:]

        near2, far2 = split_cores(mlp_in, shard_rows)
        far_gu, dgu = lax.optimization_barrier((dot_tn(far2, dgu), dgu))
        recv_gu = swap_core(far_gu)
        grad_mlp_in = dot_nt(dgu, wgu)
        part_gu = dot_tn(near2, dgu) + recv_gu
        grad_mlp_norm = jnp.sum(grad_mlp_in * normed2, axis=0)
        grad_hidden = dy.astype(jnp.float32) + norm_bwd(grad_mlp_in, normed2, norm2_inv, mlp_gain)
        hidden_b = grad_hidden.astype(jnp.bfloat16)
        hidden_b, part_gu = lax.optimization_barrier((hidden_b, part_gu))
        g_gu = scatter_chips(part_gu)

        near_h = jnp.where(core == 0, heads_rep[0], heads_rep[1])
        far_h = jnp.where(core == 0, heads_rep[1], heads_rep[0])
        recv_out = swap_core(dot_tn(far_h, hidden_b))
        grad_heads = dot_nt(hidden_b, wo).astype(jnp.bfloat16)
        part_out = dot_tn(near_h, hidden_b) + recv_out
        local_ids = (all_ids - me * rows_local).reshape(n_dev, batch, seq)
        slots = jnp.where((local_ids >= 0) & (local_ids < rows_local), local_ids, rows_local)
        grad_attn_norm, grad_q_norm, grad_k_norm = 0.0, 0.0, 0.0
        dqkv, all_rows = (), []
        for b in range(batch):
            rows = slice(b * seq, (b + 1) * seq)
            dqkv, dqg, dkg = attn_bwd(b, dqkv, qkv[b], grad_heads, cos_t, sin_t, q_gain, k_gain, batch, kv_heads, n_rep, hd)
            grad_attn_in = dot_nt(dqkv[rows], wqkv)
            grad_attn_norm += jnp.sum(grad_attn_in * normed1[b], axis=0)
            grad_q_norm += jnp.sum(dqg, axis=0)
            grad_k_norm += jnp.sum(dkg, axis=0)
            grad_x = grad_hidden[rows] + norm_bwd(grad_attn_in, normed1[b], norm1_inv[b], attn_gain)
            grad_x, dqkv = lax.optimization_barrier((row_major(grad_x), dqkv))
            all_rows.append(gather(grad_x))
            dqkv = (dqkv,)
        dqkv, = dqkv
        near1, far1 = split_cores(jnp.concatenate(attn_in, axis=0), shard_rows)
        far_qkv = dot_tn(far1, dqkv)
        part_qkv = dot_tn(near1, dqkv) + swap_core(far_qkv)
        part_tail = pack_tail(part_qkv, part_out, n_chip, kv_heads, n_rep, hd)
        g_tail = scatter_chips(part_tail)
        layer_out = (hidden.astype(jnp.float32) + dot_nn(act, wdown)).astype(jnp.bfloat16)

        vec = jnp.concatenate([grad_attn_norm, grad_mlp_norm, grad_q_norm, grad_k_norm])
        vec, layer_out, _ = lax.optimization_barrier((vec, layer_out, part_tail))
        vec = jnp.sum(lax.all_gather(vec, AXIS_NAME), axis=0)
        g_attn_norm = lax.dynamic_slice_in_dim(vec[:dim], me * shard_rows, shard_rows)
        g_mlp_norm = lax.dynamic_slice_in_dim(vec[dim:2 * dim], me * shard_rows, shard_rows)
        g_q_norm = vec[2 * dim:2 * dim + hd]
        g_k_norm = vec[2 * dim + hd:]

        d_table = jnp.zeros((rows_local, dim), jnp.float32)
        for b in range(batch):
            d_table = d_table.at[slots[:, b].reshape(-1)].add(all_rows[b], mode='drop')

        n_q = w_query.shape[1] // dim
        g_query = jnp.concatenate([g_tail[p * shard_rows:(p + 1) * shard_rows] for p in range(n_q)], axis=1)
        g_key = g_tail[n_q * shard_rows:(n_q + 1) * shard_rows]
        g_value = g_tail[(n_q + 1) * shard_rows:(n_q + 2) * shard_rows]
        g_out = g_tail[(n_q + 2) * shard_rows:]
        g_gate, g_up = unpack_gu(g_gu, n_chip)
        return (layer_out.reshape(dy_out.shape), d_table, g_attn_norm, g_query, g_key, g_value, g_q_norm, g_k_norm, g_out, g_mlp_norm, g_gate, g_up, g_down)

    return jax.shard_map(device_step, mesh=mesh, in_specs=(row_spec, row_spec, row_spec) + weight_specs + (batch_spec,), out_specs=(batch_spec, row_spec) + weight_specs, check_vma=False)
```
